512 devices in a mesh: row: 32 (over x, y), shift: 16 (over z, core).
Axes of the slice: x: 4, y: 8, z: 8, core: 2. Of those that a mesh axis runs over, the one named last changes fastest.
Arguments:
- snapshots: bfloat16 [4096, 2, 128], P('row'), may hold values from -6 to 6
- tail_sensors: bfloat16 [128, 2, 128], replicated, may hold values from -6 to 6
- shift_offsets: int32 [48], P('shift'), may hold values from 0 to 128
- start_basis: float32 [64, 4096], P(None, 'row'), may hold values from -0.09375 to 0.09375
Outputs:
- covariance: float32 [4096, 4096], P('row', 'shift')
- signal_basis: float32 [64, 4096], P(None, 'row')
The draws below stay inside these ranges and needn't reach their ends.
Inputs may be any that keep to these rules, and one draw needn't show every extreme that they name: `shift_offsets`: each shift's first sensor.
All inputs are finite; a program needn't handle non-finite values.
Results may differ from the reference program's by a relative error of at most 0.0031.
Values may be sent and summed in bfloat16 or wider, within the bound.
No kernel may reach another device: no remote copies, remote signals or barrier semaphores. Data moves between devices by JAX's collectives and lax.ppermute only.
A program may use at most 64 MiB of HBM per device.

```python
import jax
import jax.numpy as jnp
from jax import lax

M = 4096
K = 64
SNAPS = 128
TAIL = 128
ITERS = 2
SHIFTS = 48


def place_ends(drawn, stream_key, smallest, largest):
    longest = drawn.shape.index(max(drawn.shape))
    spots = []
    for shift in (0, 1):
        where = [jax.random.randint(jax.random.fold_in(stream_key, axis), (), 0, length) for axis, length in enumerate(drawn.shape)]
        where[longest] = (where[longest] + shift) % drawn.shape[longest]
        spots.append(tuple(where))
    return drawn.at[spots[0]].set(smallest).at[spots[1]].set(largest)


def level_of(rng, dims, split, low, high):
    factor_of, own = 1.0, jax.random.fold_in(rng, 6)
    for position, parts in split:
        draws = jnp.exp(jax.random.uniform(jax.random.fold_in(own, position), (parts,), jnp.float32, low / len(split), high / len(split)))
        factor_of = factor_of * jnp.repeat(draws, dims[position] // parts).reshape([-1 if axis == position else 1 for axis in range(len(dims))])
    return factor_of


def normal_values(stream_key, shape, scale, limit, split=(), held_as=jnp.bfloat16):
    factor_of = level_of(stream_key, shape, split, -0.22, 0.18) if split else 1.0
    entries = jax.random.normal(stream_key, shape, jnp.float32) * scale * factor_of
    return jnp.minimum(jnp.maximum(entries, -limit), limit).astype(held_as)


def setup_inputs(seed: int = 0) -> dict:
    splits = jax.random.split(jax.random.key(seed), 5)
    return {
        "snapshots": normal_values(splits[0], (M, 2, SNAPS), 0.7071, 6.0, ((0, 32),)),
        "tail_sensors": normal_values(splits[1], (TAIL, 2, SNAPS), 0.7071, 6.0),
        "shift_offsets": place_ends(jax.random.randint(splits[2], (SHIFTS,), 0, TAIL + 1), jax.random.fold_in(splits[2], 1), 0, TAIL).astype(jnp.int32),
        "start_basis": normal_values(splits[3], (K, M), M ** -0.5, 0.09375, ((1, 32),), jnp.float32),
    }


half_root = 0.7071067811865476

def make_rows(extended, offset):
    window = lax.dynamic_slice_in_dim(extended, offset, M, 0).astype(jnp.float32)
    mirror = window[::-1]
    summed_pair = window + mirror
    difference = window - mirror
    half_rows = M // 2
    upper_rows = jnp.concatenate([summed_pair[:half_rows, 0], summed_pair[:half_rows, 1]], axis=1)
    bottom = jnp.concatenate([difference[half_rows:, 1], -difference[half_rows:, 0]], axis=1)
    return (jnp.concatenate([upper_rows, bottom], 0) * half_root).astype(jnp.bfloat16)

def factor(gram_matrix):
    lower_factor = jnp.linalg.cholesky(gram_matrix)
    identity = jnp.eye(gram_matrix.shape[0], dtype=jnp.float32)
    return jax.scipy.linalg.solve_triangular(lower_factor, identity, lower=True)

def reference(snapshots, tail_sensors, shift_offsets, start_basis):
    extended = jnp.concatenate([snapshots, tail_sensors], 0)

    def add_shift(running, offset):
        pair_rows = make_rows(extended, offset)
        return (running + jnp.dot(pair_rows.astype(jnp.float32), pair_rows.T.astype(jnp.float32), preferred_element_type=jnp.float32), None)
    covariance_sum, unused = lax.scan(add_shift, jnp.zeros((M, M), jnp.float32), shift_offsets)
    covariance = covariance_sum * (1.0 / (SNAPS * SHIFTS))
    basis_rows = start_basis
    for sweep in range(ITERS):
        mapped = lax.dot_general(basis_rows, covariance, (((1,), (1,)), ((), ())), precision=lax.Precision.HIGHEST)
        gram_matrix = jnp.dot(mapped, mapped.T, precision=lax.Precision.HIGHEST)
        basis_rows = jnp.dot(factor(gram_matrix), mapped, precision=lax.Precision.HIGHEST)
    return (covariance, basis_rows)
```

```python
import jax
import jax.numpy as jnp
from jax import lax
from jax.experimental import pallas as pl
from jax.experimental.pallas import tpu as pltpu
from jax.sharding import Mesh
from jax.sharding import PartitionSpec as P

M = 4096
K = 64
SNAPS = 128
SHIFTS = 48
BLOCK = 128
GROUP = 4
ROW = ("row_0", "row_1")
EVERY = ("row_0", "row_1", "shift")
HALF_ROOT = 0.7071067811865476
HIGH = lax.Precision.HIGHEST


def dot_nt(a, b, precision=None):
    return lax.dot_general(
        a, b, (((1,), (1,)), ((), ())), precision=precision, preferred_element_type=jnp.float32
    )


def dot_nn(a, b, precision=None):
    return lax.dot_general(
        a, b, (((1,), (0,)), ((), ())), precision=precision, preferred_element_type=jnp.float32
    )


def sent_to_all(x, axis):
    copies = jnp.broadcast_to(x, (lax.axis_size(axis), *x.shape))
    return lax.all_to_all(copies, axis, split_axis=0, concat_axis=0, tiled=True)


def covariance_kernel(
    meta, own, after, mirror, mirror_after, tail, pieces, basis,
    cov, mapped, row_w, row_z, col_w, col_z, acc,
):
    r = meta[0]
    c = meta[1]
    flip = (
        lax.broadcasted_iota(jnp.int32, (BLOCK, BLOCK), 0)
        + lax.broadcasted_iota(jnp.int32, (BLOCK, BLOCK), 1)
        == BLOCK - 1
    ).astype(jnp.bfloat16)

    def put_window(ref, at, block, upper):
        re = block[:, :SNAPS].astype(jnp.float32) * HALF_ROOT
        im = block[:, SNAPS:].astype(jnp.float32) * HALF_ROOT
        ref[0, pl.ds(at, BLOCK), :] = jnp.where(upper, re, im)
        ref[1, pl.ds(at, BLOCK), :] = jnp.where(upper, im, -re)

    def put_mirror(ref, at, block, upper):
        turned = dot_nn(flip, block) * HALF_ROOT
        re = turned[:, :SNAPS]
        im = turned[:, SNAPS:]
        ref[0, pl.ds(at, BLOCK), :] = jnp.where(upper, re, -im)
        ref[1, pl.ds(at, BLOCK), :] = jnp.where(upper, im, re)

    row_upper = r < 16
    put_window(row_w, 0, own[...], row_upper)
    put_window(row_w, BLOCK, jnp.where(r == 31, tail[...], after[...]), row_upper)
    put_mirror(row_z, 0, jnp.where(r == 0, tail[...], mirror_after[...]), row_upper)
    put_mirror(row_z, BLOCK, mirror[...], row_upper)

    odd = [jnp.concatenate([pieces[2 * i + j, :16, :] for i in range(8)], axis=0) for j in range(2)]
    even = [jnp.concatenate([pieces[16 + 4 * i + j] for i in range(4)], axis=0) for j in range(4)]
    col_upper = c < 8
    put_window(col_w, 0, even[0], col_upper)
    put_window(col_w, BLOCK, odd[0], col_upper)
    put_window(col_w, 2 * BLOCK, jnp.where(c == 15, tail[...], even[2]), col_upper)
    put_mirror(col_z, 0, jnp.where(c == 0, tail[...], even[3]), col_upper)
    put_mirror(col_z, BLOCK, odd[1], col_upper)
    put_mirror(col_z, 2 * BLOCK, even[1], col_upper)

    acc[...] = jnp.zeros(acc.shape, jnp.float32)

    def step(at, carry):
        left, right = [], []
        for u in range(GROUP):
            o = meta[2 + at * GROUP + u]
            for plane in range(2):
                left.append(
                    (row_w[plane, pl.ds(o, BLOCK), :] + row_z[plane, pl.ds(BLOCK - o, BLOCK), :])
                    .astype(jnp.bfloat16)
                )
                right.append(
                    (col_w[plane, pl.ds(o, 2 * BLOCK), :] + col_z[plane, pl.ds(BLOCK - o, 2 * BLOCK), :])
                    .astype(jnp.bfloat16)
                )
        acc[...] += dot_nt(jnp.concatenate(left, axis=1), jnp.concatenate(right, axis=1))
        return carry

    lax.fori_loop(0, SHIFTS // GROUP, step, 0)
    block = acc[...] * (1.0 / (SNAPS * SHIFTS))
    cov[...] = block
    mapped[...] = dot_nn(basis[...], block, HIGH)


def covariance_block(meta, own, after, mirror, mirror_after, tail, pieces, basis):
    vmem = pl.BlockSpec(memory_space=pltpu.VMEM)
    return pl.pallas_call(
        covariance_kernel,
        name="covariance_block",
        in_specs=[pl.BlockSpec(memory_space=pltpu.SMEM)] + [vmem] * 7,
        out_specs=[vmem, vmem],
        out_shape=[
            jax.ShapeDtypeStruct((BLOCK, 2 * BLOCK), jnp.float32),
            jax.ShapeDtypeStruct((K, 2 * BLOCK), jnp.float32),
        ],
        scratch_shapes=[
            pltpu.VMEM((2, 2 * BLOCK, SNAPS), jnp.float32),
            pltpu.VMEM((2, 2 * BLOCK, SNAPS), jnp.float32),
            pltpu.VMEM((2, 3 * BLOCK, SNAPS), jnp.float32),
            pltpu.VMEM((2, 3 * BLOCK, SNAPS), jnp.float32),
            pltpu.VMEM((BLOCK, 2 * BLOCK), jnp.float32),
        ],
    )(meta, own, after, mirror, mirror_after, tail, pieces, basis)


def inverse_factor(gram):
    row_at = lax.broadcasted_iota(jnp.int32, (K, 2 * K), 0)
    lane_at = lax.broadcasted_iota(jnp.int32, (K, 2 * K), 1)
    eye = (lane_at == row_at + K).astype(jnp.float32)
    work = jnp.concatenate([gram, gram], axis=1)
    work = jnp.where(lane_at < K, work, eye)
    scale = jnp.zeros((K, 1), jnp.float32)
    for j in range(K):
        row = work[j : j + 1, :]
        pivot = work[j : j + 1, j : j + 1]
        factor = jnp.where(row_at[:, :1] > j, work[:, j : j + 1] / pivot, 0.0)
        scale = jnp.where(row_at[:, :1] == j, pivot, scale)
        work = work - factor * row
    return (work / jnp.sqrt(scale))[:, K:]


def image_kernel(mapped, cov, terms):
    image = mapped[...]
    terms[:, :BLOCK] = dot_nt(image, cov[...], HIGH)
    terms[:, BLOCK:] = dot_nt(image, image, HIGH)


def first_factor_kernel(total, mapped, gram):
    inverse = inverse_factor(total[:, BLOCK:])
    image = dot_nn(inverse, total[:, :BLOCK], HIGH)
    mapped[...] = image
    part = dot_nt(image, image, HIGH)
    gram[...] = jnp.concatenate([part[: K // 2], part[K // 2 :]], axis=1)


def last_factor_kernel(grams, mapped, basis):
    total = jnp.sum(grams[...], axis=0)
    gram = jnp.concatenate([total[:, :K], total[:, K:]], axis=0)
    basis[...] = dot_nn(inverse_factor(gram), mapped[...], HIGH)


def local_call(kernel, name, shapes, *operands):
    return pl.pallas_call(
        kernel,
        name=name,
        out_shape=[jax.ShapeDtypeStruct(s, jnp.float32) for s in shapes],
    )(*operands)


def total_over(terms, axis):
    n = lax.axis_size(axis)
    tiles = terms.reshape(n, terms.shape[0] // n, terms.shape[1])
    tiles = lax.all_to_all(tiles, axis, split_axis=0, concat_axis=0, tiled=True)
    return sent_to_all(tiles.sum(axis=0), axis).reshape(terms.shape)


def piece_routes():
    routes = []
    for b in range(32):
        for q in range(16):
            if b % 2:
                c = (b - 1) // 2 if q % 2 == 0 else (31 - b) // 2
                to = q
            else:
                c = (b // 2, (30 - b) // 2, (b // 2 - 1) % 16, (16 - b // 2) % 16)[q % 4]
                to = q + 16
            routes.append((b * 16 + q, to * 16 + c))
    return routes


def per_device(snapshots, tail_sensors, shift_offsets, start_basis):
    r = lax.axis_index(ROW)
    c = lax.axis_index("shift")
    own = snapshots.reshape(BLOCK, 2 * SNAPS)
    tail = tail_sensors.reshape(BLOCK, 2 * SNAPS)
    offsets = jnp.zeros((16, 2 * SNAPS), jnp.bfloat16)
    offsets = lax.dynamic_update_slice(offsets, shift_offsets.astype(jnp.bfloat16)[None], (0, 0))
    odd_piece = jnp.concatenate([lax.dynamic_slice_in_dim(own, 16 * (c // 2), 16, 0), offsets], 0)
    even_piece = lax.dynamic_slice_in_dim(own, 32 * (c // 4), 32, 0)
    piece = jnp.where(r % 2 == 1, odd_piece, even_piece)
    piece = lax.ppermute(piece, EVERY, piece_routes())
    after = lax.ppermute(own, ROW, [(i, (i - 1) % 32) for i in range(32)])
    mirror = lax.ppermute(own, ROW, [(i, 31 - i) for i in range(32)])
    mirror_after = lax.ppermute(own, ROW, [(i, (32 - i) % 32) for i in range(32)])
    pieces = sent_to_all(piece, ROW)
    every_offset = pieces[:16, 16, :3].astype(jnp.int32).reshape(-1)
    meta = jnp.concatenate([jnp.stack([r, c]).astype(jnp.int32), every_offset])
    cov, mapped = covariance_block(
        meta, own, after, mirror, mirror_after, tail, pieces, start_basis
    )
    mapped = total_over(mapped, ROW)
    (terms,) = local_call(image_kernel, "image", [(K, BLOCK + K)], mapped, cov)
    total = total_over(terms, "shift")
    mapped, gram = local_call(
        first_factor_kernel, "first_factor", [(K, BLOCK), (K // 2, 2 * K)], total
    )
    grams = sent_to_all(gram, ROW)
    (basis,) = local_call(last_factor_kernel, "last_factor", [(K, BLOCK)], grams, mapped)
    return (cov, basis)


def solution(mesh):
    split = Mesh(mesh.devices.reshape(4, 8, mesh.shape["shift"]), ("row_0", "row_1", "shift"))
    in_specs = (P(ROW, None, None), P(), P("shift"), P(None, ROW))
    out_specs = (P(ROW, "shift"), P(None, ROW))
    return jax.shard_map(
        per_device, mesh=split, in_specs=in_specs, out_specs=out_specs, check_vma=False
    )
```

```python
import jax
import jax.numpy as jnp
from jax import lax
from jax.experimental import pallas as pl
from jax.experimental.pallas import tpu as pltpu
from jax.sharding import Mesh
from jax.sharding import PartitionSpec as P

M = 4096
K = 64
SNAPS = 128
SHIFTS = 48
BLOCK = 128
GROUP = 2
ROW = ("row_0", "row_1")
EVERY = ("row_0", "row_1", "shift")
HALF_ROOT = 0.7071067811865476
HIGH = lax.Precision.HIGHEST


def dot_nt(a, b, precision=None):
    return lax.dot_general(
        a, b, (((1,), (1,)), ((), ())), precision=precision, preferred_element_type=jnp.float32
    )


def dot_nn(a, b, precision=None):
    return lax.dot_general(
        a, b, (((1,), (0,)), ((), ())), precision=precision, preferred_element_type=jnp.float32
    )


def sent_to_all(x, axis):
    copies = jnp.broadcast_to(x, (lax.axis_size(axis), *x.shape))
    return lax.all_to_all(copies, axis, split_axis=0, concat_axis=0, tiled=True)


def covariance_kernel(
    place, offsets, own, after, mirror, mirror_after, tail, pieces, basis,
    cov, mapped, row_w, row_z, col_w, col_z, acc,
):
    r = place[0]
    c = place[1]
    flip = (
        lax.broadcasted_iota(jnp.int32, (BLOCK, BLOCK), 0)
        + lax.broadcasted_iota(jnp.int32, (BLOCK, BLOCK), 1)
        == BLOCK - 1
    ).astype(jnp.bfloat16)

    def put_window(ref, at, block, upper):
        re = block[:, :SNAPS].astype(jnp.float32) * HALF_ROOT
        im = block[:, SNAPS:].astype(jnp.float32) * HALF_ROOT
        ref[0, pl.ds(at, BLOCK), :] = jnp.where(upper, re, im)
        ref[1, pl.ds(at, BLOCK), :] = jnp.where(upper, im, -re)

    def put_mirror(ref, at, block, upper):
        turned = dot_nn(flip, block) * HALF_ROOT
        re = turned[:, :SNAPS]
        im = turned[:, SNAPS:]
        ref[0, pl.ds(at, BLOCK), :] = jnp.where(upper, re, -im)
        ref[1, pl.ds(at, BLOCK), :] = jnp.where(upper, im, re)

    row_upper = r < 16
    put_window(row_w, 0, own[...], row_upper)
    put_window(row_w, BLOCK, jnp.where(r == 31, tail[...], after[...]), row_upper)
    put_mirror(row_z, 0, jnp.where(r == 0, tail[...], mirror_after[...]), row_upper)
    put_mirror(row_z, BLOCK, mirror[...], row_upper)

    odd = [jnp.concatenate([pieces[2 * i + j, :16, :] for i in range(8)], axis=0) for j in range(2)]
    even = [jnp.concatenate([pieces[16 + 4 * i + j] for i in range(4)], axis=0) for j in range(4)]
    col_upper = c < 8
    put_window(col_w, 0, even[0], col_upper)
    put_window(col_w, BLOCK, odd[0], col_upper)
    put_window(col_w, 2 * BLOCK, jnp.where(c == 15, tail[...], even[2]), col_upper)
    put_mirror(col_z, 0, jnp.where(c == 0, tail[...], even[3]), col_upper)
    put_mirror(col_z, BLOCK, odd[1], col_upper)
    put_mirror(col_z, 2 * BLOCK, even[1], col_upper)

    acc[...] = jnp.zeros(acc.shape, jnp.float32)

    def step(at, carry):
        left, right = [], []
        for u in range(3 * GROUP):
            o = offsets[at * GROUP + u // 3, u % 3]
            for plane in range(2):
                left.append(
                    (row_w[plane, pl.ds(o, BLOCK), :] + row_z[plane, pl.ds(BLOCK - o, BLOCK), :])
                    .astype(jnp.bfloat16)
                )
                right.append(
                    (col_w[plane, pl.ds(o, 2 * BLOCK), :] + col_z[plane, pl.ds(BLOCK - o, 2 * BLOCK), :])
                    .astype(jnp.bfloat16)
                )
        acc[...] += dot_nt(jnp.concatenate(left, axis=1), jnp.concatenate(right, axis=1))
        return carry

    lax.fori_loop(0, 16 // GROUP, step, 0)
    block = acc[...] * (1.0 / (SNAPS * SHIFTS))
    cov[...] = block
    image = dot_nn(basis[...], block, HIGH)
    for p in range(32):
        mapped[p] = image[4 * (p // 2) : 4 * (p // 2) + 4, SNAPS * (p % 2) : SNAPS * (p % 2) + SNAPS]


def covariance_block(place, offsets, own, after, mirror, mirror_after, tail, pieces, basis):
    vmem = pl.BlockSpec(memory_space=pltpu.VMEM)
    return pl.pallas_call(
        covariance_kernel,
        name="covariance_block",
        in_specs=[pl.BlockSpec(memory_space=pltpu.SMEM)] * 2 + [vmem] * 7,
        out_specs=[vmem, vmem],
        out_shape=[
            jax.ShapeDtypeStruct((BLOCK, 2 * BLOCK), jnp.float32),
            jax.ShapeDtypeStruct((32, 4, SNAPS), jnp.float32),
        ],
        scratch_shapes=[
            pltpu.VMEM((2, 2 * BLOCK, SNAPS), jnp.float32),
            pltpu.VMEM((2, 2 * BLOCK, SNAPS), jnp.float32),
            pltpu.VMEM((2, 3 * BLOCK, SNAPS), jnp.float32),
            pltpu.VMEM((2, 3 * BLOCK, SNAPS), jnp.float32),
            pltpu.VMEM((BLOCK, 2 * BLOCK), jnp.float32),
        ],
    )(place, offsets, own, after, mirror, mirror_after, tail, pieces, basis)


def inverse_factor(gram):
    row_at = lax.broadcasted_iota(jnp.int32, (8, 2 * K), 0)
    lane_at = lax.broadcasted_iota(jnp.int32, (8, 2 * K), 1)
    tiles, done = [], []
    for t in range(K // 8):
        part = gram[8 * t : 8 * t + 8]
        eye = (lane_at == row_at + (K + 8 * t)).astype(jnp.float32)
        tiles.append(jnp.where(lane_at < K, jnp.concatenate([part, part], axis=1), eye))
        done.append(jnp.zeros((8, 2 * K), jnp.float32))
    for j in range(K):
        at, s = divmod(j, 8)
        row = tiles[at][s : s + 1, :]
        cols = [jnp.broadcast_to(tiles[t][:, j : j + 1], (8, 2 * K)) for t in range(at, K // 8)]
        pivot = cols[0][s : s + 1, :]
        scaled = row * (1.0 / pivot)
        done[at] = jnp.where(row_at == s, row / jnp.sqrt(pivot), done[at])
        tiles[at] = jnp.where(row_at > s, tiles[at] - cols[0] * scaled, tiles[at])
        for t in range(at + 1, K // 8):
            tiles[t] = tiles[t] - cols[t - at] * scaled
    return jnp.concatenate(done, axis=0)[:, K:]


def image_kernel(mapped, cov, terms):
    image = jnp.concatenate(
        [jnp.concatenate([mapped[2 * i], mapped[2 * i + 1]], axis=1) for i in range(16)], axis=0
    )
    product = dot_nt(image, cov[...], HIGH)
    gram = dot_nt(image, image, HIGH)
    gram = jnp.concatenate([gram, gram], axis=1)
    for t in range(8):
        terms[2 * t] = product[8 * t : 8 * t + 8]
        terms[2 * t + 1] = gram[8 * t : 8 * t + 8]


def first_factor_kernel(total, mapped, grams):
    product = jnp.concatenate([total[2 * t] for t in range(8)], axis=0)
    gram = jnp.concatenate([total[2 * t + 1] for t in range(8)], axis=0)
    image = dot_nn(inverse_factor(gram[:, :K]), product, HIGH)
    mapped[...] = image
    part = dot_nt(image, image, HIGH)
    part = jnp.concatenate([part[: K // 2], part[K // 2 :]], axis=1)
    for i in range(grams.shape[0]):
        grams[i] = part


def last_factor_kernel(grams, mapped, basis):
    total = jnp.sum(grams[...], axis=0)
    gram = jnp.concatenate([total[:, :K], total[:, K:]], axis=0)
    basis[...] = dot_nn(inverse_factor(gram), mapped[...], HIGH)


def local_call(kernel, name, shapes, *operands):
    return pl.pallas_call(
        kernel,
        name=name,
        out_shape=[jax.ShapeDtypeStruct(s, jnp.float32) for s in shapes],
    )(*operands)


def exchanged(tiles, axis):
    return lax.all_to_all(tiles, axis, split_axis=0, concat_axis=0, tiled=True)


def total_over(tiles, axis):
    return sent_to_all(exchanged(tiles, axis).sum(axis=0), axis)


def piece_routes():
    routes = []
    for b in range(32):
        for q in range(16):
            if b % 2:
                c = (b - 1) // 2 if q % 2 == 0 else (31 - b) // 2
                to = q
            else:
                c = (b // 2, (30 - b) // 2, (b // 2 - 1) % 16, (16 - b // 2) % 16)[q % 4]
                to = q + 16
            routes.append((b * 16 + q, to * 16 + c))
    return routes


def per_device(snapshots, tail_sensors, shift_offsets, start_basis):
    r = lax.axis_index(ROW)
    c = lax.axis_index("shift")
    own = snapshots.reshape(BLOCK, 2 * SNAPS)
    tail = tail_sensors.reshape(BLOCK, 2 * SNAPS)
    offsets = jnp.zeros((16, 2 * SNAPS), jnp.bfloat16)
    offsets = lax.dynamic_update_slice(offsets, shift_offsets.astype(jnp.bfloat16)[None], (0, 0))
    odd_piece = jnp.concatenate([lax.dynamic_slice_in_dim(own, 16 * (c // 2), 16, 0), offsets], 0)
    even_piece = lax.dynamic_slice_in_dim(own, 32 * (c // 4), 32, 0)
    piece = jnp.where(r % 2 == 1, odd_piece, even_piece)
    piece = lax.ppermute(piece, EVERY, piece_routes())
    after = lax.ppermute(own, ROW, [(i, (i - 1) % 32) for i in range(32)])
    mirror = lax.ppermute(own, ROW, [(i, 31 - i) for i in range(32)])
    mirror_after = lax.ppermute(own, ROW, [(i, (32 - i) % 32) for i in range(32)])
    pieces = sent_to_all(piece, ROW)
    every_offset = pieces[:16, 16, :3].astype(jnp.int32)
    place = jnp.stack([r, c]).astype(jnp.int32)
    cov, mapped = covariance_block(
        place, every_offset, own, after, mirror, mirror_after, tail, pieces, start_basis
    )
    mapped = total_over(mapped, ROW)
    (terms,) = local_call(image_kernel, "image", [(16, 8, SNAPS)], mapped, cov)
    total = total_over(terms, "shift")
    mapped, grams = local_call(
        first_factor_kernel, "first_factor", [(K, BLOCK), (4, K // 2, 2 * K)], total
    )
    grams = sent_to_all(exchanged(grams, "row_0").sum(axis=0), "row_1")
    (basis,) = local_call(last_factor_kernel, "last_factor", [(K, BLOCK)], grams, mapped)
    return (cov, basis)


def solution(mesh):
    split = Mesh(mesh.devices.reshape(4, 8, mesh.shape["shift"]), ("row_0", "row_1", "shift"))
    in_specs = (P(ROW, None, None), P(), P("shift"), P(None, ROW))
    out_specs = (P(ROW, "shift"), P(None, ROW))
    return jax.shard_map(
        per_device, mesh=split, in_specs=in_specs, out_specs=out_specs, check_vma=False
    )
```

```python
import jax
import jax.numpy as jnp
from jax import lax
from jax.experimental import pallas as pl
from jax.experimental.pallas import tpu as pltpu
from jax.sharding import Mesh
from jax.sharding import PartitionSpec as P


K = 64
SNAPS = 128
SHIFTS = 48
BLOCK = 128
GROUP = 2
ROW = ("row_0", "row_1")
EVERY = ("row_0", "row_1", "shift")
HALF_ROOT = 0.7071067811865476
HIGH = lax.Precision.HIGHEST


def dot_nt(a, b, precision=None):
    return lax.dot_general(
        a, b, (((1,), (1,)), ((), ())), precision=precision, preferred_element_type=jnp.float32
    )


def dot_nn(a, b, precision=None):
    return lax.dot_general(
        a, b, (((1,), (0,)), ((), ())), precision=precision, preferred_element_type=jnp.float32
    )


def sent_to_all(x, axis):
    copies = jnp.broadcast_to(x, (lax.axis_size(axis), *x.shape))
    return lax.all_to_all(copies, axis, split_axis=0, concat_axis=0, tiled=True)


def covariance_kernel(
    place, offsets, own, after, mirror, mirror_after, tail, pieces, basis,
    cov, mapped, row_w, row_z, col_w, col_z, acc,
):
    r = place[0]
    c = place[1]
    flip = (
        lax.broadcasted_iota(jnp.int32, (BLOCK, BLOCK), 0)
        + lax.broadcasted_iota(jnp.int32, (BLOCK, BLOCK), 1)
        == BLOCK - 1
    ).astype(jnp.bfloat16)

    def put_window(ref, at, block, upper):
        re = block[:, :SNAPS].astype(jnp.float32) * HALF_ROOT
        im = block[:, SNAPS:].astype(jnp.float32) * HALF_ROOT
        ref[0, pl.ds(at, BLOCK), :] = jnp.where(upper, re, im)
        ref[1, pl.ds(at, BLOCK), :] = jnp.where(upper, im, -re)

    def put_mirror(ref, at, block, upper):
        turned = dot_nn(flip, block) * HALF_ROOT
        re = turned[:, :SNAPS]
        im = turned[:, SNAPS:]
        ref[0, pl.ds(at, BLOCK), :] = jnp.where(upper, re, -im)
        ref[1, pl.ds(at, BLOCK), :] = jnp.where(upper, im, re)

    row_upper = r < 16
    put_window(row_w, 0, own[...], row_upper)
    put_window(row_w, BLOCK, jnp.where(r == 31, tail[...], after[...]), row_upper)
    put_mirror(row_z, 0, jnp.where(r == 0, tail[...], mirror_after[...]), row_upper)
    put_mirror(row_z, BLOCK, mirror[...], row_upper)

    odd = [jnp.concatenate([pieces[2 * i + j, :16, :] for i in range(8)], axis=0) for j in range(2)]
    even = [jnp.concatenate([pieces[16 + 4 * i + j] for i in range(4)], axis=0) for j in range(4)]
    col_upper = c < 8
    put_window(col_w, 0, even[0], col_upper)
    put_window(col_w, BLOCK, odd[0], col_upper)
    put_window(col_w, 2 * BLOCK, jnp.where(c == 15, tail[...], even[2]), col_upper)
    put_mirror(col_z, 0, jnp.where(c == 0, tail[...], even[3]), col_upper)
    put_mirror(col_z, BLOCK, odd[1], col_upper)
    put_mirror(col_z, 2 * BLOCK, even[1], col_upper)

    acc[...] = jnp.zeros(acc.shape, jnp.float32)

    def step(at, carry):
        left, right = [], []
        for u in range(3 * GROUP):
            o = offsets[at * GROUP + u // 3, u % 3]
            for plane in range(2):
                left.append(
                    (row_w[plane, pl.ds(o, BLOCK), :] + row_z[plane, pl.ds(BLOCK - o, BLOCK), :])
                    .astype(jnp.bfloat16)
                )
                right.append(
                    (col_w[plane, pl.ds(o, 2 * BLOCK), :] + col_z[plane, pl.ds(BLOCK - o, 2 * BLOCK), :])
                    .astype(jnp.bfloat16)
                )
        acc[...] += dot_nt(jnp.concatenate(left, axis=1), jnp.concatenate(right, axis=1))
        return carry

    lax.fori_loop(0, 16 // GROUP, step, 0)
    block = acc[...] * (1.0 / (SNAPS * SHIFTS))
    cov[...] = block
    image = dot_nn(basis[...], block, HIGH)
    for p in range(32):
        mapped[p] = image[4 * (p // 2) : 4 * (p // 2) + 4, SNAPS * (p % 2) : SNAPS * (p % 2) + SNAPS]


def covariance_block(place, offsets, own, after, mirror, mirror_after, tail, pieces, basis):
    vmem = pl.BlockSpec(memory_space=pltpu.VMEM)
    return pl.pallas_call(
        covariance_kernel,
        name="covariance_block",
        in_specs=[pl.BlockSpec(memory_space=pltpu.SMEM)] * 2 + [vmem] * 7,
        out_specs=[vmem, vmem],
        out_shape=[
            jax.ShapeDtypeStruct((BLOCK, 2 * BLOCK), jnp.float32),
            jax.ShapeDtypeStruct((32, 4, SNAPS), jnp.float32),
        ],
        scratch_shapes=[
            pltpu.VMEM((2, 2 * BLOCK, SNAPS), jnp.float32),
            pltpu.VMEM((2, 2 * BLOCK, SNAPS), jnp.float32),
            pltpu.VMEM((2, 3 * BLOCK, SNAPS), jnp.float32),
            pltpu.VMEM((2, 3 * BLOCK, SNAPS), jnp.float32),
            pltpu.VMEM((BLOCK, 2 * BLOCK), jnp.float32),
        ],
    )(place, offsets, own, after, mirror, mirror_after, tail, pieces, basis)


def inverse_factor(gram):
    row_at = lax.broadcasted_iota(jnp.int32, (8, 2 * K), 0)
    lane_at = lax.broadcasted_iota(jnp.int32, (8, 2 * K), 1)
    tiles, done = [], []
    for t in range(K // 8):
        part = gram[8 * t : 8 * t + 8]
        eye = (lane_at == row_at + (K + 8 * t)).astype(jnp.float32)
        tiles.append(jnp.where(lane_at < K, jnp.concatenate([part, part], axis=1), eye))
        done.append(jnp.zeros((8, 2 * K), jnp.float32))
    for at in range(K // 8):
        own, rest = at, range(at + 1, K // 8)
        cols = [
            [jnp.broadcast_to(tiles[t][:, j : j + 1], (8, 2 * K)) for t in range(at, K // 8)]
            for j in range(8 * at, 8 * at + 8)
        ]
        for s in range(8):
            col = cols[s]
            below = row_at > s
            pivot = col[0][s : s + 1, :]
            inverse = 1.0 / pivot
            row = tiles[own][s : s + 1, :]
            scaled = row * inverse
            done[own] = jnp.where(row_at == s, row / jnp.sqrt(pivot), done[own])
            for k in range(s + 1, 8):
                share = cols[k][0][s : s + 1, :] * inverse
                left = [c - f * share for c, f in zip(cols[k], col)]
                left[0] = jnp.where(below, left[0], cols[k][0])
                cols[k] = left
            tiles[own] = jnp.where(below, tiles[own] - col[0] * scaled, tiles[own])
            for t in rest:
                tiles[t] = tiles[t] - col[t - at] * scaled
    return jnp.concatenate(done, axis=0)[:, K:]


def image_kernel(mapped, cov, terms):
    image = jnp.concatenate(
        [jnp.concatenate([mapped[2 * i], mapped[2 * i + 1]], axis=1) for i in range(16)], axis=0
    )
    product = dot_nt(image, cov[...], HIGH)
    gram = dot_nt(image, image, HIGH)
    gram = jnp.concatenate([gram, gram], axis=1)
    for t in range(8):
        terms[2 * t] = product[8 * t : 8 * t + 8]
        terms[2 * t + 1] = gram[8 * t : 8 * t + 8]


def first_factor_kernel(total, mapped, grams):
    product = jnp.concatenate([total[2 * t] for t in range(8)], axis=0)
    gram = jnp.concatenate([total[2 * t + 1] for t in range(8)], axis=0)
    image = dot_nn(inverse_factor(gram[:, :K]), product, HIGH)
    mapped[...] = image
    part = dot_nt(image, image, HIGH)
    part = jnp.concatenate([part[: K // 2], part[K // 2 :]], axis=1)
    for i in range(grams.shape[0]):
        grams[i] = part


def last_factor_kernel(grams, mapped, basis):
    total = jnp.sum(grams[...], axis=0)
    gram = jnp.concatenate([total[:, :K], total[:, K:]], axis=0)
    basis[...] = dot_nn(inverse_factor(gram), mapped[...], HIGH)


def local_call(kernel, shapes, *operands):
    return pl.pallas_call(
        kernel, out_shape=[jax.ShapeDtypeStruct(s, jnp.float32) for s in shapes]
    )(*operands)


def exchanged(tiles, axis):
    return lax.all_to_all(tiles, axis, split_axis=0, concat_axis=0, tiled=True)


def total_over(tiles, axis):
    return sent_to_all(exchanged(tiles, axis).sum(axis=0), axis)


def piece_routes():
    routes = []
    for b in range(32):
        for q in range(16):
            if b % 2:
                c = (b - 1) // 2 if q % 2 == 0 else (31 - b) // 2
                to = q
            else:
                c = (b // 2, (30 - b) // 2, (b // 2 - 1) % 16, (16 - b // 2) % 16)[q % 4]
                to = q + 16
            routes.append((b * 16 + q, to * 16 + c))
    return routes


def per_device(snapshots, tail_sensors, shift_offsets, start_basis):
    r = lax.axis_index(ROW)
    c = lax.axis_index("shift")
    own = snapshots.reshape(BLOCK, 2 * SNAPS)
    tail = tail_sensors.reshape(BLOCK, 2 * SNAPS)
    offsets = jnp.zeros((16, 2 * SNAPS), jnp.bfloat16)
    offsets = lax.dynamic_update_slice(offsets, shift_offsets.astype(jnp.bfloat16)[None], (0, 0))
    odd_piece = jnp.concatenate([lax.dynamic_slice_in_dim(own, 16 * (c // 2), 16, 0), offsets], 0)
    even_piece = lax.dynamic_slice_in_dim(own, 32 * (c // 4), 32, 0)
    piece = jnp.where(r % 2 == 1, odd_piece, even_piece)
    piece = lax.ppermute(piece, EVERY, piece_routes())
    after = lax.ppermute(own, ROW, [(i, (i - 1) % 32) for i in range(32)])
    mirror = lax.ppermute(own, ROW, [(i, 31 - i) for i in range(32)])
    mirror_after = lax.ppermute(own, ROW, [(i, (32 - i) % 32) for i in range(32)])
    pieces = sent_to_all(piece, ROW)
    every_offset = pieces[:16, 16, :3].astype(jnp.int32)
    place = jnp.stack([r, c]).astype(jnp.int32)
    cov, mapped = covariance_block(
        place, every_offset, own, after, mirror, mirror_after, tail, pieces, start_basis
    )
    mapped = total_over(mapped, ROW)
    (terms,) = local_call(image_kernel, [(16, 8, SNAPS)], mapped, cov)
    total = total_over(terms, "shift")
    mapped, grams = local_call(first_factor_kernel, [(K, BLOCK), (4, K // 2, 2 * K)], total)
    grams = sent_to_all(exchanged(grams, "row_0").sum(axis=0), "row_1")
    (basis,) = local_call(last_factor_kernel, [(K, BLOCK)], grams, mapped)
    return (cov, basis)


def solution(mesh):
    split = Mesh(mesh.devices.reshape(4, 8, mesh.shape["shift"]), ("row_0", "row_1", "shift"))
    in_specs = (P(ROW, None, None), P(), P("shift"), P(None, ROW))
    out_specs = (P(ROW, "shift"), P(None, ROW))
    return jax.shard_map(
        per_device, mesh=split, in_specs=in_specs, out_specs=out_specs, check_vma=False
    )
```

```python
import jax
import jax.numpy as jnp
from jax import lax
from jax.experimental import pallas as pl
from jax.experimental.pallas import tpu as pltpu
from jax.sharding import Mesh
from jax.sharding import PartitionSpec as P


K = 64
SNAPS = 128
SHIFTS = 48
BLOCK = 128
GROUP = 2
ROW = ("row_0", "row_1")
SHIFT = ("z", "core")
EVERY = (*ROW, *SHIFT)
HALF_ROOT = 0.7071067811865476
HIGH = lax.Precision.HIGHEST


def dot_nt(a, b, precision=None):
    return lax.dot_general(
        a, b, (((1,), (1,)), ((), ())), precision=precision, preferred_element_type=jnp.float32
    )


def dot_nn(a, b, precision=None):
    return lax.dot_general(
        a, b, (((1,), (0,)), ((), ())), precision=precision, preferred_element_type=jnp.float32
    )


def sent_to_all(x, axis):
    copies = jnp.broadcast_to(x, (lax.axis_size(axis), *x.shape))
    return lax.all_to_all(copies, axis, split_axis=0, concat_axis=0, tiled=True)


def covariance_kernel(
    place, offsets, own, after, mirror, mirror_after, tail, pieces, basis,
    cov, mapped, row_w, row_z, col_w, col_z, acc,
):
    r = place[0]
    c = place[1]
    flip = (
        lax.broadcasted_iota(jnp.int32, (BLOCK, BLOCK), 0)
        + lax.broadcasted_iota(jnp.int32, (BLOCK, BLOCK), 1)
        == BLOCK - 1
    ).astype(jnp.bfloat16)

    def put_window(ref, at, block, upper):
        re = block[:, :SNAPS].astype(jnp.float32) * HALF_ROOT
        im = block[:, SNAPS:].astype(jnp.float32) * HALF_ROOT
        ref[0, pl.ds(at, BLOCK), :] = jnp.where(upper, re, im)
        ref[1, pl.ds(at, BLOCK), :] = jnp.where(upper, im, -re)

    def put_mirror(ref, at, block, upper):
        turned = dot_nn(flip, block) * HALF_ROOT
        re = turned[:, :SNAPS]
        im = turned[:, SNAPS:]
        ref[0, pl.ds(at, BLOCK), :] = jnp.where(upper, re, -im)
        ref[1, pl.ds(at, BLOCK), :] = jnp.where(upper, im, re)

    row_upper = r < 16
    put_window(row_w, 0, own[...], row_upper)
    put_window(row_w, BLOCK, jnp.where(r == 31, tail[...], after[...]), row_upper)
    put_mirror(row_z, 0, jnp.where(r == 0, tail[...], mirror_after[...]), row_upper)
    put_mirror(row_z, BLOCK, mirror[...], row_upper)

    odd = [jnp.concatenate([pieces[2 * i + j, :16, :] for i in range(8)], axis=0) for j in range(2)]
    even = [jnp.concatenate([pieces[16 + 4 * i + j] for i in range(4)], axis=0) for j in range(4)]
    col_upper = c < 8
    put_window(col_w, 0, even[0], col_upper)
    put_window(col_w, BLOCK, odd[0], col_upper)
    put_window(col_w, 2 * BLOCK, jnp.where(c == 15, tail[...], even[2]), col_upper)
    put_mirror(col_z, 0, jnp.where(c == 0, tail[...], even[3]), col_upper)
    put_mirror(col_z, BLOCK, odd[1], col_upper)
    put_mirror(col_z, 2 * BLOCK, even[1], col_upper)

    acc[...] = jnp.zeros(acc.shape, jnp.float32)

    def step(at, carry):
        left, right = [], []
        for u in range(3 * GROUP):
            o = offsets[at * GROUP + u // 3, u % 3]
            for plane in range(2):
                left.append(
                    (row_w[plane, pl.ds(o, BLOCK), :] + row_z[plane, pl.ds(BLOCK - o, BLOCK), :])
                    .astype(jnp.bfloat16)
                )
                right.append(
                    (col_w[plane, pl.ds(o, 2 * BLOCK), :] + col_z[plane, pl.ds(BLOCK - o, 2 * BLOCK), :])
                    .astype(jnp.bfloat16)
                )
        acc[...] += dot_nt(jnp.concatenate(left, axis=1), jnp.concatenate(right, axis=1))
        return carry

    lax.fori_loop(0, 16 // GROUP, step, 0)
    block = acc[...] * (1.0 / (SNAPS * SHIFTS))
    cov[...] = block
    image = dot_nn(basis[...], block, HIGH)
    for p in range(32):
        mapped[p] = image[4 * (p // 2) : 4 * (p // 2) + 4, SNAPS * (p % 2) : SNAPS * (p % 2) + SNAPS]


def covariance_block(place, offsets, own, after, mirror, mirror_after, tail, pieces, basis):
    vmem = pl.BlockSpec(memory_space=pltpu.VMEM)
    return pl.pallas_call(
        covariance_kernel,
        name="covariance_block",
        in_specs=[pl.BlockSpec(memory_space=pltpu.SMEM)] * 2 + [vmem] * 7,
        out_specs=[vmem, vmem],
        out_shape=[
            jax.ShapeDtypeStruct((BLOCK, 2 * BLOCK), jnp.float32),
            jax.ShapeDtypeStruct((32, 4, SNAPS), jnp.float32),
        ],
        scratch_shapes=[
            pltpu.VMEM((2, 2 * BLOCK, SNAPS), jnp.float32),
            pltpu.VMEM((2, 2 * BLOCK, SNAPS), jnp.float32),
            pltpu.VMEM((2, 3 * BLOCK, SNAPS), jnp.float32),
            pltpu.VMEM((2, 3 * BLOCK, SNAPS), jnp.float32),
            pltpu.VMEM((BLOCK, 2 * BLOCK), jnp.float32),
        ],
    )(place, offsets, own, after, mirror, mirror_after, tail, pieces, basis)


def inverse_factor(gram):
    row_at = lax.broadcasted_iota(jnp.int32, (8, 2 * K), 0)
    lane_at = lax.broadcasted_iota(jnp.int32, (8, 2 * K), 1)
    tiles, done = [], []
    for t in range(K // 8):
        part = gram[8 * t : 8 * t + 8]
        eye = (lane_at == row_at + (K + 8 * t)).astype(jnp.float32)
        tiles.append(jnp.where(lane_at < K, jnp.concatenate([part, part], axis=1), eye))
        done.append(jnp.zeros((8, 2 * K), jnp.float32))
    for at in range(K // 8):
        own, rest = at, range(at + 1, K // 8)
        cols = [
            [jnp.broadcast_to(tiles[t][:, j : j + 1], (8, 2 * K)) for t in range(at, K // 8)]
            for j in range(8 * at, 8 * at + 8)
        ]
        for s in range(8):
            col = cols[s]
            below = row_at > s
            pivot = col[0][s : s + 1, :]
            inverse = 1.0 / pivot
            row = tiles[own][s : s + 1, :]
            scaled = row * inverse
            done[own] = jnp.where(row_at == s, row / jnp.sqrt(pivot), done[own])
            for k in range(s + 1, 8):
                share = cols[k][0][s : s + 1, :] * inverse
                left = [c - f * share for c, f in zip(cols[k], col)]
                left[0] = jnp.where(below, left[0], cols[k][0])
                cols[k] = left
            tiles[own] = jnp.where(below, tiles[own] - col[0] * scaled, tiles[own])
            for t in rest:
                tiles[t] = tiles[t] - col[t - at] * scaled
    return jnp.concatenate(done, axis=0)[:, K:]


def image_kernel(place, mapped, cov, kept, sent):
    image = jnp.concatenate(
        [jnp.concatenate([mapped[2 * i], mapped[2 * i + 1]], axis=1) for i in range(16)], axis=0
    )
    product = dot_nt(image, cov[...], HIGH)
    gram = dot_nt(image, image, HIGH)
    terms = jnp.concatenate([product, halves_side_by_side(gram)], axis=0)
    half = terms.shape[0] // 2
    first = place[1] % 2 == 0
    kept[...] = jnp.where(first, terms[:half], terms[half:])
    sent[...] = jnp.where(first, terms[half:], terms[:half])


def halves_side_by_side(gram):
    return jnp.concatenate([gram[: K // 2], gram[K // 2 :]], axis=1)


def halves_stacked(packed):
    return jnp.concatenate([packed[:, :K], packed[:, K:]], axis=0)


def first_factor_kernel(place, mine, other, mapped, grams):
    first = place[1] % 2 == 0
    total = jnp.concatenate(
        [jnp.where(first, mine[...], other[...]), jnp.where(first, other[...], mine[...])], axis=0
    )
    image = dot_nn(inverse_factor(halves_stacked(total[K:])), total[:K], HIGH)
    mapped[...] = image
    part = halves_side_by_side(dot_nt(image, image, HIGH))
    for i in range(grams.shape[0]):
        grams[i] = part


def last_factor_kernel(grams, mapped, basis):
    total = jnp.sum(grams[...], axis=0)
    basis[...] = dot_nn(inverse_factor(halves_stacked(total)), mapped[...], HIGH)


def local_call(kernel, shapes, *operands):
    spaces = [pltpu.SMEM if x.dtype == jnp.int32 else pltpu.VMEM for x in operands]
    return pl.pallas_call(
        kernel,
        in_specs=[pl.BlockSpec(memory_space=space) for space in spaces],
        out_shape=[jax.ShapeDtypeStruct(s, jnp.float32) for s in shapes],
    )(*operands)


def exchanged(tiles, axis):
    return lax.all_to_all(tiles, axis, split_axis=0, concat_axis=0, tiled=True)


def total_over(tiles, axis):
    return sent_to_all(exchanged(tiles, axis).sum(axis=0), axis)


def piece_routes():
    routes = []
    for b in range(32):
        for q in range(16):
            if b % 2:
                c = (b - 1) // 2 if q % 2 == 0 else (31 - b) // 2
                to = q
            else:
                c = (b // 2, (30 - b) // 2, (b // 2 - 1) % 16, (16 - b // 2) % 16)[q % 4]
                to = q + 16
            routes.append((b * 16 + q, to * 16 + c))
    return routes


def per_device(snapshots, tail_sensors, shift_offsets, start_basis):
    r = lax.axis_index(ROW)
    c = lax.axis_index(SHIFT)
    own = snapshots.reshape(BLOCK, 2 * SNAPS)
    tail = tail_sensors.reshape(BLOCK, 2 * SNAPS)
    offsets = jnp.zeros((16, 2 * SNAPS), jnp.bfloat16)
    offsets = lax.dynamic_update_slice(offsets, shift_offsets.astype(jnp.bfloat16)[None], (0, 0))
    odd_piece = jnp.concatenate([lax.dynamic_slice_in_dim(own, 16 * (c // 2), 16, 0), offsets], 0)
    even_piece = lax.dynamic_slice_in_dim(own, 32 * (c // 4), 32, 0)
    piece = jnp.where(r % 2 == 1, odd_piece, even_piece)
    piece = lax.ppermute(piece, EVERY, piece_routes())
    after = lax.ppermute(own, ROW, [(i, (i - 1) % 32) for i in range(32)])
    mirror = lax.ppermute(own, ROW, [(i, 31 - i) for i in range(32)])
    mirror_after = lax.ppermute(own, ROW, [(i, (32 - i) % 32) for i in range(32)])
    pieces = sent_to_all(piece, "row_1")
    pieces = sent_to_all(pieces, "row_0").reshape(32, 32, 2 * SNAPS)
    every_offset = pieces[:16, 16, :3].astype(jnp.int32)
    place = jnp.stack([r, c]).astype(jnp.int32)
    cov, mapped = covariance_block(
        place, every_offset, own, after, mirror, mirror_after, tail, pieces, start_basis
    )
    mapped = total_over(mapped, ROW)
    half = (3 * K // 4, BLOCK)
    kept, sent = local_call(image_kernel, [half, half], place, mapped, cov)
    swap = [(0, 1), (1, 0)]
    mine = sent_to_all(kept + lax.ppermute(sent, "core", swap), "z").sum(axis=0)
    other = lax.ppermute(mine, "core", swap)
    mapped, grams = local_call(
        first_factor_kernel, [(K, BLOCK), (4, K // 2, 2 * K)], place, mine, other
    )
    grams = sent_to_all(exchanged(grams, "row_0").sum(axis=0), "row_1")
    (basis,) = local_call(last_factor_kernel, [(K, BLOCK)], grams, mapped)
    return (cov, basis)


def solution(mesh):
    split = Mesh(mesh.devices.reshape(4, 8, 8, 2), EVERY)
    in_specs = (P(ROW, None, None), P(), P(SHIFT), P(None, ROW))
    out_specs = (P(ROW, SHIFT), P(None, ROW))
    return jax.shard_map(
        per_device, mesh=split, in_specs=in_specs, out_specs=out_specs, check_vma=False
    )
```

```python
import jax
import jax.numpy as jnp
from jax import lax
from jax.experimental import pallas as pl
from jax.experimental.pallas import tpu as pltpu
from jax.sharding import Mesh
from jax.sharding import PartitionSpec as P

M = 4096
K = 64
SNAPS = 128
SHIFTS = 48
BLOCK = 128
GROUP = 2
ROW = ("row_0", "row_1")
SHIFT = ("z", "core")
EVERY = (*ROW, *SHIFT)
HALF_ROOT = 0.7071067811865476
HIGH = lax.Precision.HIGHEST


def dot_nt(a, b, precision=None):
    return lax.dot_general(
        a, b, (((1,), (1,)), ((), ())), precision=precision, preferred_element_type=jnp.float32
    )


def dot_nn(a, b, precision=None):
    return lax.dot_general(
        a, b, (((1,), (0,)), ((), ())), precision=precision, preferred_element_type=jnp.float32
    )


def sent_to_all(x, axis):
    copies = jnp.broadcast_to(x, (lax.axis_size(axis), *x.shape))
    return lax.all_to_all(copies, axis, split_axis=0, concat_axis=0, tiled=True)


def covariance_kernel(
    place, offsets, own, after, mirror, mirror_after, tail, pieces, basis,
    cov, mapped, row_w, row_z, col_w, col_z, acc,
):
    r = place[0]
    c = place[1]
    flip = (
        lax.broadcasted_iota(jnp.int32, (BLOCK, BLOCK), 0)
        + lax.broadcasted_iota(jnp.int32, (BLOCK, BLOCK), 1)
        == BLOCK - 1
    ).astype(jnp.bfloat16)

    def put_window(ref, at, block, upper):
        re = block[:, :SNAPS].astype(jnp.float32) * HALF_ROOT
        im = block[:, SNAPS:].astype(jnp.float32) * HALF_ROOT
        ref[0, pl.ds(at, BLOCK), :] = jnp.where(upper, re, im)
        ref[1, pl.ds(at, BLOCK), :] = jnp.where(upper, im, -re)

    def put_mirror(ref, at, block, upper):
        turned = dot_nn(flip, block) * HALF_ROOT
        re = turned[:, :SNAPS]
        im = turned[:, SNAPS:]
        ref[0, pl.ds(at, BLOCK), :] = jnp.where(upper, re, -im)
        ref[1, pl.ds(at, BLOCK), :] = jnp.where(upper, im, re)

    row_upper = r < 16
    put_window(row_w, 0, own[:BLOCK], row_upper)
    put_window(row_w, BLOCK, jnp.where(r == 31, tail[...], after[:BLOCK]), row_upper)
    put_mirror(row_z, 0, jnp.where(r == 0, tail[...], mirror_after[:BLOCK]), row_upper)
    put_mirror(row_z, BLOCK, mirror[:BLOCK], row_upper)

    odd = [pieces[0, :BLOCK], pieces[1, :BLOCK]]
    even = [pieces[2, :BLOCK], pieces[3, :BLOCK], pieces[0, BLOCK : 2 * BLOCK], pieces[1, BLOCK : 2 * BLOCK]]
    col_upper = c < 8
    put_window(col_w, 0, even[0], col_upper)
    put_window(col_w, BLOCK, odd[0], col_upper)
    put_window(col_w, 2 * BLOCK, jnp.where(c == 15, tail[...], even[2]), col_upper)
    put_mirror(col_z, 0, jnp.where(c == 0, tail[...], even[3]), col_upper)
    put_mirror(col_z, BLOCK, odd[1], col_upper)
    put_mirror(col_z, 2 * BLOCK, even[1], col_upper)

    acc[...] = jnp.zeros(acc.shape, jnp.float32)

    def step(at, carry):
        left, right = [], []
        for u in range(3 * GROUP):
            o = offsets[at * GROUP + u // 3, u % 3]
            for plane in range(2):
                left.append(
                    (row_w[plane, pl.ds(o, BLOCK), :] + row_z[plane, pl.ds(BLOCK - o, BLOCK), :])
                    .astype(jnp.bfloat16)
                )
                right.append(
                    (col_w[plane, pl.ds(o, 2 * BLOCK), :] + col_z[plane, pl.ds(BLOCK - o, 2 * BLOCK), :])
                    .astype(jnp.bfloat16)
                )
        acc[...] += dot_nt(jnp.concatenate(left, axis=1), jnp.concatenate(right, axis=1))
        return carry

    lax.fori_loop(0, 16 // GROUP, step, 0)
    block = acc[...] * (1.0 / (SNAPS * SHIFTS))
    cov[...] = block
    image = dot_nn(basis[...], block, HIGH)
    for p in range(32):
        mapped[p] = image[4 * (p // 2) : 4 * (p // 2) + 4, SNAPS * (p % 2) : SNAPS * (p % 2) + SNAPS]


def covariance_block(place, offsets, own, after, mirror, mirror_after, tail, pieces, basis):
    vmem = pl.BlockSpec(memory_space=pltpu.VMEM)
    return pl.pallas_call(
        covariance_kernel,
        name="covariance_block",
        in_specs=[pl.BlockSpec(memory_space=pltpu.SMEM)] * 2 + [vmem] * 7,
        out_specs=[vmem, vmem],
        out_shape=[
            jax.ShapeDtypeStruct((BLOCK, 2 * BLOCK), jnp.float32),
            jax.ShapeDtypeStruct((32, 4, SNAPS), jnp.float32),
        ],
        scratch_shapes=[
            pltpu.VMEM((2, 2 * BLOCK, SNAPS), jnp.float32),
            pltpu.VMEM((2, 2 * BLOCK, SNAPS), jnp.float32),
            pltpu.VMEM((2, 3 * BLOCK, SNAPS), jnp.float32),
            pltpu.VMEM((2, 3 * BLOCK, SNAPS), jnp.float32),
            pltpu.VMEM((BLOCK, 2 * BLOCK), jnp.float32),
        ],
    )(place, offsets, own, after, mirror, mirror_after, tail, pieces, basis)


def inverse_factor(gram):
    row_at = lax.broadcasted_iota(jnp.int32, (8, 2 * K), 0)
    lane_at = lax.broadcasted_iota(jnp.int32, (8, 2 * K), 1)
    tiles, done = [], []
    for t in range(K // 8):
        part = gram[8 * t : 8 * t + 8]
        eye = (lane_at == row_at + (K + 8 * t)).astype(jnp.float32)
        tiles.append(jnp.where(lane_at < K, jnp.concatenate([part, part], axis=1), eye))
        done.append(jnp.zeros((8, 2 * K), jnp.float32))
    for at in range(K // 8):
        own, rest = at, range(at + 1, K // 8)
        cols = [
            [jnp.broadcast_to(tiles[t][:, j : j + 1], (8, 2 * K)) for t in range(at, K // 8)]
            for j in range(8 * at, 8 * at + 8)
        ]
        for s in range(8):
            col = cols[s]
            below = row_at > s
            pivot = col[0][s : s + 1, :]
            inverse = 1.0 / pivot
            row = tiles[own][s : s + 1, :]
            scaled = row * inverse
            done[own] = jnp.where(row_at == s, row / jnp.sqrt(pivot), done[own])
            for k in range(s + 1, 8):
                share = cols[k][0][s : s + 1, :] * inverse
                left = [c - f * share for c, f in zip(cols[k], col)]
                left[0] = jnp.where(below, left[0], cols[k][0])
                cols[k] = left
            tiles[own] = jnp.where(below, tiles[own] - col[0] * scaled, tiles[own])
            for t in rest:
                tiles[t] = tiles[t] - col[t - at] * scaled
    return jnp.concatenate(done, axis=0)[:, K:]


def image_kernel(place, mapped, cov, kept, sent):
    image = jnp.concatenate(
        [jnp.concatenate([mapped[2 * i], mapped[2 * i + 1]], axis=1) for i in range(16)], axis=0
    )
    product = dot_nt(image, cov[...], HIGH)
    gram = dot_nt(image, image, HIGH)
    terms = jnp.concatenate([product, halves_side_by_side(gram)], axis=0)
    half = terms.shape[0] // 2
    first = place[1] % 2 == 0
    kept[...] = jnp.where(first, terms[:half], terms[half:])
    sent[...] = jnp.where(first, terms[half:], terms[:half])


def halves_side_by_side(gram):
    return jnp.concatenate([gram[: K // 2], gram[K // 2 :]], axis=1)


def halves_stacked(packed):
    return jnp.concatenate([packed[:, :K], packed[:, K:]], axis=0)


def first_factor_kernel(place, mine, other, mapped, grams):
    first = place[1] % 2 == 0
    total = jnp.concatenate(
        [jnp.where(first, mine[...], other[...]), jnp.where(first, other[...], mine[...])], axis=0
    )
    image = dot_nn(inverse_factor(halves_stacked(total[K:])), total[:K], HIGH)
    mapped[...] = image
    part = halves_side_by_side(dot_nt(image, image, HIGH))
    for i in range(grams.shape[0]):
        grams[i] = part


def last_factor_kernel(grams, mapped, basis):
    total = jnp.sum(grams[...], axis=0)
    basis[...] = dot_nn(inverse_factor(halves_stacked(total)), mapped[...], HIGH)


def local_call(kernel, name, shapes, *operands):
    spaces = [pltpu.SMEM if x.dtype == jnp.int32 else pltpu.VMEM for x in operands]
    return pl.pallas_call(
        kernel,
        name=name,
        in_specs=[pl.BlockSpec(memory_space=space) for space in spaces],
        out_shape=[jax.ShapeDtypeStruct(s, jnp.float32) for s in shapes],
    )(*operands)


def exchanged(tiles, axis):
    return lax.all_to_all(tiles, axis, split_axis=0, concat_axis=0, tiled=True)


def total_over(tiles, axis):
    return sent_to_all(exchanged(tiles, axis).sum(axis=0), axis)


def routes(source):
    pairs = []
    for x in range(4):
        for y in range(8):
            for c in range(16):
                b, q = source(x, y, c)
                pairs.append((b % 32 * 16 + q % 16, (x * 8 + y) * 16 + c))
    return pairs


def first_columns(x, y, c):
    return (2 * c + 1, 31 - 2 * c, 2 * c, 30 - 2 * c)[x], c + 2 * (y + x)


def second_columns(x, y, c):
    return (2 * c + 2, 32 - 2 * c, 2 * c + 1, 31 - 2 * c)[x], c + 2 * (y + x + 4)


def rows_after(x, y, c):
    return 8 * x + y + 1, c + 2 * x + 1


def rows_mirror(x, y, c):
    return 31 - 8 * x - y, c + 2 * x + 9


def rows_mirror_after(x, y, c):
    return 32 - 8 * x - y, c


def per_device(snapshots, tail_sensors, shift_offsets, start_basis):
    r = lax.axis_index(ROW)
    c = lax.axis_index(SHIFT)
    own = snapshots.reshape(BLOCK, 2 * SNAPS)
    tail = tail_sensors.reshape(BLOCK, 2 * SNAPS)
    offsets = jnp.zeros((8, 2 * SNAPS), jnp.bfloat16)
    offsets = lax.dynamic_update_slice(offsets, shift_offsets.astype(jnp.bfloat16)[None], (0, 0))
    own = jnp.concatenate([own, offsets], axis=0)
    first, second, after, mirror, mirror_after = (
        lax.ppermute(own, EVERY, routes(source))
        for source in (first_columns, second_columns, rows_after, rows_mirror, rows_mirror_after)
    )
    held = [first[:BLOCK], second[:BLOCK]] + [m[BLOCK:] for m in (first, second, after, mirror)]
    pieces = sent_to_all(jnp.concatenate(held, axis=0), "row_0")
    every_offset = pieces[:, 2 * BLOCK :: 8, :3].astype(jnp.int32).reshape(16, 3)
    place = jnp.stack([r, c]).astype(jnp.int32)
    cov, mapped = covariance_block(
        place, every_offset, own, after, mirror, mirror_after, tail, pieces, start_basis
    )
    mapped = total_over(mapped, ROW)
    half = (3 * K // 4, BLOCK)
    kept, sent = local_call(image_kernel, "image", [half, half], place, mapped, cov)
    swap = [(0, 1), (1, 0)]
    mine = sent_to_all(kept + lax.ppermute(sent, "core", swap), "z").sum(axis=0)
    other = lax.ppermute(mine, "core", swap)
    mapped, grams = local_call(
        first_factor_kernel, "first_factor", [(K, BLOCK), (4, K // 2, 2 * K)], place, mine, other
    )
    grams = sent_to_all(exchanged(grams, "row_0").sum(axis=0), "row_1")
    (basis,) = local_call(last_factor_kernel, "last_factor", [(K, BLOCK)], grams, mapped)
    return (cov, basis)


def solution(mesh):
    split = Mesh(mesh.devices.reshape(4, 8, 8, 2), EVERY)
    in_specs = (P(ROW, None, None), P(), P(SHIFT), P(None, ROW))
    out_specs = (P(ROW, SHIFT), P(None, ROW))
    step = jax.shard_map(
        per_device, mesh=split, in_specs=in_specs, out_specs=out_specs, check_vma=False
    )
    return step
```

```python
import jax
import jax.numpy as jnp
from jax import lax
from jax.experimental import pallas as pl
from jax.experimental.pallas import tpu as pltpu
from jax.sharding import Mesh
from jax.sharding import PartitionSpec as P


K = 64
SNAPS = 128
SHIFTS = 48
BLOCK = 128
GROUP = 16
ROW = ("row_0", "row_1")
SHIFT = ("z", "core")
EVERY = (*ROW, *SHIFT)
HALF_ROOT = 0.7071067811865476
HIGH = lax.Precision.HIGHEST


def dot_nt(a, b, precision=None):
    return lax.dot_general(
        a, b, (((1,), (1,)), ((), ())), precision=precision, preferred_element_type=jnp.float32
    )


def dot_nn(a, b, precision=None):
    return lax.dot_general(
        a, b, (((1,), (0,)), ((), ())), precision=precision, preferred_element_type=jnp.float32
    )


def near(x):
    return pltpu.with_memory_space_constraint(x, pltpu.VMEM)


def sent_to_all(x, axis):
    copies = jnp.broadcast_to(x, (lax.axis_size(axis), *x.shape))
    return lax.all_to_all(copies, axis, split_axis=0, concat_axis=0, tiled=True)


def covariance_kernel(
    place, offsets, own, after, mirror, mirror_after, tail, pieces, basis,
    cov, cov_near, mapped, row_w, row_z, col_w, col_z, acc,
):
    r = place[0]
    c = place[1]
    flip = (
        lax.broadcasted_iota(jnp.int32, (BLOCK, BLOCK), 0)
        + lax.broadcasted_iota(jnp.int32, (BLOCK, BLOCK), 1)
        == BLOCK - 1
    ).astype(jnp.bfloat16)

    def put_window(ref, at, block, upper):
        re = block[:, :SNAPS].astype(jnp.float32) * HALF_ROOT
        im = block[:, SNAPS:].astype(jnp.float32) * HALF_ROOT
        ref[0, pl.ds(at, BLOCK), :] = jnp.where(upper, re, im)
        ref[1, pl.ds(at, BLOCK), :] = jnp.where(upper, im, -re)

    def put_mirror(ref, at, block, upper):
        turned = dot_nn(flip, block) * HALF_ROOT
        re = turned[:, :SNAPS]
        im = turned[:, SNAPS:]
        ref[0, pl.ds(at, BLOCK), :] = jnp.where(upper, re, -im)
        ref[1, pl.ds(at, BLOCK), :] = jnp.where(upper, im, re)

    row_upper = r < 16
    put_window(row_w, 0, own[...], row_upper)
    put_window(row_w, BLOCK, jnp.where(r == 31, tail[...], after[...]), row_upper)
    put_mirror(row_z, 0, jnp.where(r == 0, tail[...], mirror_after[...]), row_upper)
    put_mirror(row_z, BLOCK, mirror[...], row_upper)

    odd = [jnp.concatenate([pieces[2 * i + j, :16, :] for i in range(8)], axis=0) for j in range(2)]
    even = [jnp.concatenate([pieces[16 + 4 * i + j] for i in range(4)], axis=0) for j in range(4)]
    col_upper = c < 8
    put_window(col_w, 0, even[0], col_upper)
    put_window(col_w, BLOCK, odd[0], col_upper)
    put_window(col_w, 2 * BLOCK, jnp.where(c == 15, tail[...], even[2]), col_upper)
    put_mirror(col_z, 0, jnp.where(c == 0, tail[...], even[3]), col_upper)
    put_mirror(col_z, BLOCK, odd[1], col_upper)
    put_mirror(col_z, 2 * BLOCK, even[1], col_upper)

    acc[...] = jnp.zeros(acc.shape, jnp.float32)

    def step(at, carry):
        left, right = [], []
        for u in range(3 * GROUP):
            o = offsets[at * GROUP + u // 3, u % 3]
            for plane in range(2):
                left.append(
                    (row_w[plane, pl.ds(o, BLOCK), :] + row_z[plane, pl.ds(BLOCK - o, BLOCK), :])
                    .astype(jnp.bfloat16)
                )
                right.append(
                    (col_w[plane, pl.ds(o, 2 * BLOCK), :] + col_z[plane, pl.ds(BLOCK - o, 2 * BLOCK), :])
                    .astype(jnp.bfloat16)
                )
        acc[...] += dot_nt(jnp.concatenate(left, axis=1), jnp.concatenate(right, axis=1))
        return carry

    step(0, 0)
    block = acc[...] * (1.0 / (SNAPS * SHIFTS))
    cov[...] = block
    cov_near[...] = block
    image = dot_nn(basis[...], block, HIGH)
    for p in range(32):
        mapped[p] = image[4 * (p // 2) : 4 * (p // 2) + 4, SNAPS * (p % 2) : SNAPS * (p % 2) + SNAPS]


def covariance_block(place, offsets, own, after, mirror, mirror_after, tail, pieces, basis):
    vmem = pl.BlockSpec(memory_space=pltpu.VMEM)
    return pl.pallas_call(
        covariance_kernel,
        name="covariance_block",
        in_specs=[pl.BlockSpec(memory_space=pltpu.SMEM)] * 2 + [vmem] * 7,
        out_specs=[vmem] * 3,
        out_shape=[
            jax.ShapeDtypeStruct((BLOCK, 2 * BLOCK), jnp.float32),
            pltpu.VMEM((BLOCK, 2 * BLOCK), jnp.float32),
            pltpu.VMEM((32, 4, SNAPS), jnp.float32),
        ],
        scratch_shapes=[
            pltpu.VMEM((2, 2 * BLOCK, SNAPS), jnp.float32),
            pltpu.VMEM((2, 2 * BLOCK, SNAPS), jnp.float32),
            pltpu.VMEM((2, 3 * BLOCK, SNAPS), jnp.float32),
            pltpu.VMEM((2, 3 * BLOCK, SNAPS), jnp.float32),
            pltpu.VMEM((BLOCK, 2 * BLOCK), jnp.float32),
        ],
    )(place, offsets, *[near(x) for x in (own, after, mirror, mirror_after, tail, pieces, basis)])


def inverse_factor(gram):
    row_at = lax.broadcasted_iota(jnp.int32, (8, 2 * K), 0)
    lane_at = lax.broadcasted_iota(jnp.int32, (8, 2 * K), 1)
    tiles, done = [], []
    for t in range(K // 8):
        part = gram[8 * t : 8 * t + 8]
        eye = (lane_at == row_at + (K + 8 * t)).astype(jnp.float32)
        tiles.append(jnp.where(lane_at < K, jnp.concatenate([part, part], axis=1), eye))
        done.append(jnp.zeros((8, 2 * K), jnp.float32))
    for at in range(K // 8):
        own, rest = at, range(at + 1, K // 8)
        cols = [
            [jnp.broadcast_to(tiles[t][:, j : j + 1], (8, 2 * K)) for t in range(at, K // 8)]
            for j in range(8 * at, 8 * at + 8)
        ]
        for s in range(8):
            col = cols[s]
            below = row_at > s
            pivot = col[0][s : s + 1, :]
            inverse = 1.0 / pivot
            row = tiles[own][s : s + 1, :]
            scaled = row * inverse
            done[own] = jnp.where(row_at == s, row / jnp.sqrt(pivot), done[own])
            for k in range(s + 1, 8):
                share = cols[k][0][s : s + 1, :] * inverse
                left = [c - f * share for c, f in zip(cols[k], col)]
                left[0] = jnp.where(below, left[0], cols[k][0])
                cols[k] = left
            tiles[own] = jnp.where(below, tiles[own] - col[0] * scaled, tiles[own])
            for t in rest:
                tiles[t] = tiles[t] - col[t - at] * scaled
    return jnp.concatenate(done, axis=0)[:, K:]


def image_kernel(place, mapped, cov, kept, sent):
    image = jnp.concatenate(
        [jnp.concatenate([mapped[2 * i], mapped[2 * i + 1]], axis=1) for i in range(16)], axis=0
    )
    product = dot_nt(image, cov[...], HIGH)
    gram = dot_nt(image, image, HIGH)
    terms = jnp.concatenate([product, halves_side_by_side(gram)], axis=0)
    half = terms.shape[0] // 2
    first = place[1] % 2 == 0
    kept[...] = jnp.where(first, terms[:half], terms[half:])
    sent[...] = jnp.where(first, terms[half:], terms[:half])


def halves_side_by_side(gram):
    return jnp.concatenate([gram[: K // 2], gram[K // 2 :]], axis=1)


def halves_stacked(packed):
    return jnp.concatenate([packed[:, :K], packed[:, K:]], axis=0)


def first_factor_kernel(place, mine, other, mapped, grams):
    first = place[1] % 2 == 0
    total = jnp.concatenate(
        [jnp.where(first, mine[...], other[...]), jnp.where(first, other[...], mine[...])], axis=0
    )
    image = dot_nn(inverse_factor(halves_stacked(total[K:])), total[:K], HIGH)
    mapped[...] = image
    part = halves_side_by_side(dot_nt(image, image, HIGH))
    for i in range(grams.shape[0]):
        grams[i] = part


def last_factor_kernel(grams, mapped, basis):
    total = jnp.sum(grams[...], axis=0)
    basis[...] = dot_nn(inverse_factor(halves_stacked(total)), mapped[...], HIGH)


def local_call(kernel, shapes, *operands, result=pltpu.VMEM):
    spaces = [pltpu.SMEM if x.dtype == jnp.int32 else pltpu.VMEM for x in operands]
    return pl.pallas_call(
        kernel,
        in_specs=[pl.BlockSpec(memory_space=space) for space in spaces],
        out_shape=[result(s, jnp.float32) for s in shapes],
    )(*[x if x.dtype == jnp.int32 else near(x) for x in operands])


def exchanged(tiles, axis):
    return lax.all_to_all(tiles, axis, split_axis=0, concat_axis=0, tiled=True)


def total_over(tiles, axis):
    return sent_to_all(exchanged(tiles, axis).sum(axis=0), axis)


def piece_routes():
    routes = []
    for b in range(32):
        for q in range(16):
            if b % 2:
                c = (b - 1) // 2 if q % 2 == 0 else (31 - b) // 2
                to = q
            else:
                c = (b // 2, (30 - b) // 2, (b // 2 - 1) % 16, (16 - b // 2) % 16)[q % 4]
                to = q + 16
            routes.append((b * 16 + q, to * 16 + c))
    return routes


def per_device(snapshots, tail_sensors, shift_offsets, start_basis):
    r = lax.axis_index(ROW)
    c = lax.axis_index(SHIFT)
    own = snapshots.reshape(BLOCK, 2 * SNAPS)
    tail = tail_sensors.reshape(BLOCK, 2 * SNAPS)
    offsets = jnp.zeros((16, 2 * SNAPS), jnp.bfloat16)
    offsets = lax.dynamic_update_slice(offsets, shift_offsets.astype(jnp.bfloat16)[None], (0, 0))
    odd_piece = jnp.concatenate([lax.dynamic_slice_in_dim(own, 16 * (c // 2), 16, 0), offsets], 0)
    even_piece = lax.dynamic_slice_in_dim(own, 32 * (c // 4), 32, 0)
    piece = jnp.where(r % 2 == 1, odd_piece, even_piece)
    piece = lax.ppermute(piece, EVERY, piece_routes())
    after = lax.ppermute(own, ROW, [(i, (i - 1) % 32) for i in range(32)])
    mirror = lax.ppermute(own, ROW, [(i, 31 - i) for i in range(32)])
    mirror_after = lax.ppermute(own, ROW, [(i, (32 - i) % 32) for i in range(32)])
    pieces = sent_to_all(piece, ROW)
    every_offset = pieces[:16, 16, :3].astype(jnp.int32)
    place = jnp.stack([r, c]).astype(jnp.int32)
    cov, cov_near, mapped = covariance_block(
        place, every_offset, own, after, mirror, mirror_after, tail, pieces, start_basis
    )
    mapped = total_over(mapped, ROW)
    half = (3 * K // 4, BLOCK)
    kept, sent = local_call(image_kernel, [half, half], place, mapped, cov_near)
    swap = [(0, 1), (1, 0)]
    mine = sent_to_all(kept + lax.ppermute(sent, "core", swap), "z").sum(axis=0)
    other = lax.ppermute(mine, "core", swap)
    mapped, grams = local_call(
        first_factor_kernel, [(K, BLOCK), (4, K // 2, 2 * K)], place, mine, other
    )
    grams = sent_to_all(exchanged(grams, "row_0").sum(axis=0), "row_1")
    (basis,) = local_call(last_factor_kernel, [(K, BLOCK)], grams, mapped, result=jax.ShapeDtypeStruct)
    return (cov, basis)


def solution(mesh):
    split = Mesh(mesh.devices.reshape(4, 8, 8, 2), EVERY)
    in_specs = (P(ROW, None, None), P(), P(SHIFT), P(None, ROW))
    out_specs = (P(ROW, SHIFT), P(None, ROW))
    return jax.shard_map(
        per_device, mesh=split, in_specs=in_specs, out_specs=out_specs, check_vma=False
    )
```

```python
import jax
import jax.numpy as jnp
from jax import lax
from jax.experimental import pallas as pl
from jax.experimental.pallas import tpu as pltpu
from jax.sharding import Mesh
from jax.sharding import PartitionSpec as P


K = 64
SNAPS = 128
SHIFTS = 48
BLOCK = 128
GROUP = 16
ROW = ("row_0", "row_1")
SHIFT = ("z", "core")
EVERY = (*ROW, *SHIFT)
HALF_ROOT = 0.7071067811865476
HIGH = lax.Precision.HIGHEST


def dot_nt(a, b, precision=None):
    return lax.dot_general(
        a, b, (((1,), (1,)), ((), ())), precision=precision, preferred_element_type=jnp.float32
    )


def dot_nn(a, b, precision=None):
    return lax.dot_general(
        a, b, (((1,), (0,)), ((), ())), precision=precision, preferred_element_type=jnp.float32
    )


def near(x):
    return pltpu.with_memory_space_constraint(x, pltpu.VMEM)


def sent_to_all(x, axis):
    copies = jnp.broadcast_to(x, (lax.axis_size(axis), *x.shape))
    return lax.all_to_all(copies, axis, split_axis=0, concat_axis=0, tiled=True)


def copies_kernel(piece, copies):
    for i in range(copies.shape[0]):
        copies[i] = piece[...]


def copies_of(piece, count):
    return pl.pallas_call(
        copies_kernel, name="copies", out_shape=pltpu.VMEM((count, *piece.shape), piece.dtype)
    )(near(piece))


def covariance_kernel(
    place, offsets, own, after, mirror, mirror_after, tail, pieces, basis,
    cov, cov_near, mapped, row_w, row_z, col_w, col_z, acc,
):
    r = place[0]
    c = place[1]
    flip = (
        lax.broadcasted_iota(jnp.int32, (BLOCK, BLOCK), 0)
        + lax.broadcasted_iota(jnp.int32, (BLOCK, BLOCK), 1)
        == BLOCK - 1
    ).astype(jnp.bfloat16)

    def put_window(ref, at, block, upper):
        re = block[:, :SNAPS].astype(jnp.float32) * HALF_ROOT
        im = block[:, SNAPS:].astype(jnp.float32) * HALF_ROOT
        ref[0, pl.ds(at, BLOCK), :] = jnp.where(upper, re, im)
        ref[1, pl.ds(at, BLOCK), :] = jnp.where(upper, im, -re)

    def put_mirror(ref, at, block, upper):
        turned = dot_nn(flip, block) * HALF_ROOT
        re = turned[:, :SNAPS]
        im = turned[:, SNAPS:]
        ref[0, pl.ds(at, BLOCK), :] = jnp.where(upper, re, -im)
        ref[1, pl.ds(at, BLOCK), :] = jnp.where(upper, im, re)

    row_upper = r < 16
    put_window(row_w, 0, own[...], row_upper)
    put_window(row_w, BLOCK, jnp.where(r == 31, tail[...], after[...]), row_upper)
    put_mirror(row_z, 0, jnp.where(r == 0, tail[...], mirror_after[...]), row_upper)
    put_mirror(row_z, BLOCK, mirror[...], row_upper)

    odd = [jnp.concatenate([pieces[2 * i + j, :16, :] for i in range(8)], axis=0) for j in range(2)]
    even = [jnp.concatenate([pieces[16 + 4 * i + j] for i in range(4)], axis=0) for j in range(4)]
    col_upper = c < 8
    put_window(col_w, 0, even[0], col_upper)
    put_window(col_w, BLOCK, odd[0], col_upper)
    put_window(col_w, 2 * BLOCK, jnp.where(c == 15, tail[...], even[2]), col_upper)
    put_mirror(col_z, 0, jnp.where(c == 0, tail[...], even[3]), col_upper)
    put_mirror(col_z, BLOCK, odd[1], col_upper)
    put_mirror(col_z, 2 * BLOCK, even[1], col_upper)

    acc[...] = jnp.zeros(acc.shape, jnp.float32)

    def step(at, carry):
        left, right = [], []
        for u in range(3 * GROUP):
            o = offsets[at * GROUP + u // 3, u % 3]
            for plane in range(2):
                left.append(
                    (row_w[plane, pl.ds(o, BLOCK), :] + row_z[plane, pl.ds(BLOCK - o, BLOCK), :])
                    .astype(jnp.bfloat16)
                )
                right.append(
                    (col_w[plane, pl.ds(o, 2 * BLOCK), :] + col_z[plane, pl.ds(BLOCK - o, 2 * BLOCK), :])
                    .astype(jnp.bfloat16)
                )
        acc[...] += dot_nt(jnp.concatenate(left, axis=1), jnp.concatenate(right, axis=1))
        return carry

    step(0, 0)
    block = acc[...] * (1.0 / (SNAPS * SHIFTS))
    cov[...] = block
    cov_near[...] = block
    image = dot_nn(basis[...], block, HIGH)
    for p in range(32):
        mapped[p] = image[4 * (p // 2) : 4 * (p // 2) + 4, SNAPS * (p % 2) : SNAPS * (p % 2) + SNAPS]


def covariance_block(place, offsets, own, after, mirror, mirror_after, tail, pieces, basis):
    vmem = pl.BlockSpec(memory_space=pltpu.VMEM)
    return pl.pallas_call(
        covariance_kernel,
        name="covariance_block",
        in_specs=[pl.BlockSpec(memory_space=pltpu.SMEM)] * 2 + [vmem] * 7,
        out_specs=[vmem] * 3,
        out_shape=[
            jax.ShapeDtypeStruct((BLOCK, 2 * BLOCK), jnp.float32),
            pltpu.VMEM((BLOCK, 2 * BLOCK), jnp.float32),
            pltpu.VMEM((32, 4, SNAPS), jnp.float32),
        ],
        scratch_shapes=[
            pltpu.VMEM((2, 2 * BLOCK, SNAPS), jnp.float32),
            pltpu.VMEM((2, 2 * BLOCK, SNAPS), jnp.float32),
            pltpu.VMEM((2, 3 * BLOCK, SNAPS), jnp.float32),
            pltpu.VMEM((2, 3 * BLOCK, SNAPS), jnp.float32),
            pltpu.VMEM((BLOCK, 2 * BLOCK), jnp.float32),
        ],
    )(place, offsets, *[near(x) for x in (own, after, mirror, mirror_after, tail, pieces, basis)])


def inverse_factor(gram):
    row_at = lax.broadcasted_iota(jnp.int32, (8, 2 * K), 0)
    lane_at = lax.broadcasted_iota(jnp.int32, (8, 2 * K), 1)
    tiles, done = [], []
    for t in range(K // 8):
        part = gram[8 * t : 8 * t + 8]
        eye = (lane_at == row_at + (K + 8 * t)).astype(jnp.float32)
        tiles.append(jnp.where(lane_at < K, jnp.concatenate([part, part], axis=1), eye))
        done.append(jnp.zeros((8, 2 * K), jnp.float32))
    for at in range(K // 8):
        own, rest = at, range(at + 1, K // 8)
        cols = [
            [jnp.broadcast_to(tiles[t][:, j : j + 1], (8, 2 * K)) for t in range(at, K // 8)]
            for j in range(8 * at, 8 * at + 8)
        ]
        for s in range(8):
            col = cols[s]
            below = row_at > s
            pivot = col[0][s : s + 1, :]
            inverse = 1.0 / pivot
            row = tiles[own][s : s + 1, :]
            scaled = row * inverse
            done[own] = jnp.where(row_at == s, row / jnp.sqrt(pivot), done[own])
            for k in range(s + 1, 8):
                share = cols[k][0][s : s + 1, :] * inverse
                left = [c - f * share for c, f in zip(cols[k], col)]
                left[0] = jnp.where(below, left[0], cols[k][0])
                cols[k] = left
            tiles[own] = jnp.where(below, tiles[own] - col[0] * scaled, tiles[own])
            for t in rest:
                tiles[t] = tiles[t] - col[t - at] * scaled
    return jnp.concatenate(done, axis=0)[:, K:]


def image_kernel(place, mapped, cov, kept, sent):
    image = jnp.concatenate(
        [jnp.concatenate([mapped[2 * i], mapped[2 * i + 1]], axis=1) for i in range(16)], axis=0
    )
    product = dot_nt(image, cov[...], HIGH)
    gram = dot_nt(image, image, HIGH)
    terms = jnp.concatenate([product, halves_side_by_side(gram)], axis=0)
    half = terms.shape[0] // 2
    first = place[1] % 2 == 0
    kept[...] = jnp.where(first, terms[:half], terms[half:])
    sent[...] = jnp.where(first, terms[half:], terms[:half])


def halves_side_by_side(gram):
    return jnp.concatenate([gram[: K // 2], gram[K // 2 :]], axis=1)


def halves_stacked(packed):
    return jnp.concatenate([packed[:, :K], packed[:, K:]], axis=0)


def first_factor_kernel(place, mine, other, mapped, grams):
    first = place[1] % 2 == 0
    total = jnp.concatenate(
        [jnp.where(first, mine[...], other[...]), jnp.where(first, other[...], mine[...])], axis=0
    )
    image = dot_nn(inverse_factor(halves_stacked(total[K:])), total[:K], HIGH)
    mapped[...] = image
    part = halves_side_by_side(dot_nt(image, image, HIGH))
    for i in range(grams.shape[0]):
        grams[i] = part


def last_factor_kernel(grams, mapped, basis):
    total = jnp.sum(grams[...], axis=0)
    basis[...] = dot_nn(inverse_factor(halves_stacked(total)), mapped[...], HIGH)


def local_call(kernel, shapes, *operands, result=pltpu.VMEM):
    spaces = [pltpu.SMEM if x.dtype == jnp.int32 else pltpu.VMEM for x in operands]
    return pl.pallas_call(
        kernel,
        in_specs=[pl.BlockSpec(memory_space=space) for space in spaces],
        out_shape=[result(s, jnp.float32) for s in shapes],
    )(*[x if x.dtype == jnp.int32 else near(x) for x in operands])


def exchanged(tiles, axis):
    return lax.all_to_all(tiles, axis, split_axis=0, concat_axis=0, tiled=True)


def total_over(tiles, axis):
    return sent_to_all(exchanged(tiles, axis).sum(axis=0), axis)


def piece_routes():
    routes = []
    for b in range(32):
        for q in range(16):
            if b % 2:
                c = (b - 1) // 2 if q % 2 == 0 else (31 - b) // 2
                to = q
            else:
                c = (b // 2, (30 - b) // 2, (b // 2 - 1) % 16, (16 - b // 2) % 16)[q % 4]
                to = q + 16
            routes.append((b * 16 + q, to * 16 + c))
    return routes


def per_device(snapshots, tail_sensors, shift_offsets, start_basis):
    r = lax.axis_index(ROW)
    c = lax.axis_index(SHIFT)
    own = snapshots.reshape(BLOCK, 2 * SNAPS)
    tail = tail_sensors.reshape(BLOCK, 2 * SNAPS)
    offsets = jnp.zeros((16, 2 * SNAPS), jnp.bfloat16)
    offsets = lax.dynamic_update_slice(offsets, shift_offsets.astype(jnp.bfloat16)[None], (0, 0))
    odd_piece = jnp.concatenate([lax.dynamic_slice_in_dim(own, 16 * (c // 2), 16, 0), offsets], 0)
    even_piece = lax.dynamic_slice_in_dim(own, 32 * (c // 4), 32, 0)
    piece = jnp.where(r % 2 == 1, odd_piece, even_piece)
    piece = lax.ppermute(piece, EVERY, piece_routes())
    after = lax.ppermute(own, ROW, [(i, (i - 1) % 32) for i in range(32)])
    mirror = lax.ppermute(own, ROW, [(i, 31 - i) for i in range(32)])
    mirror_after = lax.ppermute(own, ROW, [(i, (32 - i) % 32) for i in range(32)])
    pieces = exchanged(copies_of(piece, lax.axis_size(ROW)), ROW)
    every_offset = pieces[:16, 16, :3].astype(jnp.int32)
    place = jnp.stack([r, c]).astype(jnp.int32)
    cov, cov_near, mapped = covariance_block(
        place, every_offset, own, after, mirror, mirror_after, tail, pieces, start_basis
    )
    mapped = total_over(mapped, ROW)
    half = (3 * K // 4, BLOCK)
    kept, sent = local_call(image_kernel, [half, half], place, mapped, cov_near)
    swap = [(0, 1), (1, 0)]
    mine = sent_to_all(kept + lax.ppermute(sent, "core", swap), "z").sum(axis=0)
    other = lax.ppermute(mine, "core", swap)
    mapped, grams = local_call(
        first_factor_kernel, [(K, BLOCK), (4, K // 2, 2 * K)], place, mine, other
    )
    grams = sent_to_all(exchanged(grams, "row_0").sum(axis=0), "row_1")
    (basis,) = local_call(last_factor_kernel, [(K, BLOCK)], grams, mapped, result=jax.ShapeDtypeStruct)
    return (cov, basis)


def solution(mesh):
    split = Mesh(mesh.devices.reshape(4, 8, 8, 2), EVERY)
    in_specs = (P(ROW, None, None), P(), P(SHIFT), P(None, ROW))
    out_specs = (P(ROW, SHIFT), P(None, ROW))
    return jax.shard_map(
        per_device, mesh=split, in_specs=in_specs, out_specs=out_specs, check_vma=False
    )
```

```python
import jax
import jax.numpy as jnp
from jax import lax
from jax.experimental import pallas as pl
from jax.experimental.pallas import tpu as pltpu
from jax.sharding import Mesh
from jax.sharding import PartitionSpec as P


K = 64
SNAPS = 128
SHIFTS = 48
BLOCK = 128
GROUP = 16
ROW = ("row_0", "row_1")
SHIFT = ("z", "core")
EVERY = (*ROW, *SHIFT)
HALF_ROOT = 0.7071067811865476
HIGH = lax.Precision.HIGHEST
CORES_SWAPPED = [(0, 1), (1, 0)]


def dot_nt(a, b, precision=None):
    return lax.dot_general(
        a, b, (((1,), (1,)), ((), ())), precision=precision, preferred_element_type=jnp.float32
    )


def dot_nn(a, b, precision=None):
    return lax.dot_general(
        a, b, (((1,), (0,)), ((), ())), precision=precision, preferred_element_type=jnp.float32
    )


def near(x):
    return pltpu.with_memory_space_constraint(x, pltpu.VMEM)


def sent_to_all(x, axis):
    copies = jnp.broadcast_to(x, (lax.axis_size(axis), *x.shape))
    return lax.all_to_all(copies, axis, split_axis=0, concat_axis=0, tiled=True)


def covariance_kernel(
    place, offsets, own, mine, other, tail, pieces, basis,
    cov, cov_near, mapped, row_w, row_z, col_w, col_z, acc,
):
    r = place[0]
    c = place[1]
    flip = (
        lax.broadcasted_iota(jnp.int32, (BLOCK, BLOCK), 0)
        + lax.broadcasted_iota(jnp.int32, (BLOCK, BLOCK), 1)
        == BLOCK - 1
    ).astype(jnp.bfloat16)

    def put_window(ref, at, block, upper):
        re = block[:, :SNAPS].astype(jnp.float32) * HALF_ROOT
        im = block[:, SNAPS:].astype(jnp.float32) * HALF_ROOT
        ref[0, pl.ds(at, BLOCK), :] = jnp.where(upper, re, im)
        ref[1, pl.ds(at, BLOCK), :] = jnp.where(upper, im, -re)

    def put_mirror(ref, at, block, upper):
        turned = dot_nn(flip, block) * HALF_ROOT
        re = turned[:, :SNAPS]
        im = turned[:, SNAPS:]
        ref[0, pl.ds(at, BLOCK), :] = jnp.where(upper, re, -im)
        ref[1, pl.ds(at, BLOCK), :] = jnp.where(upper, im, re)

    first = c % 2 == 0
    after, mirror, mirror_after = (
        jnp.concatenate(
            [jnp.where(first, mine[i], other[i]), jnp.where(first, other[i], mine[i])], axis=0
        )
        for i in range(3)
    )
    row_upper = r < 16
    put_window(row_w, 0, own[...], row_upper)
    put_window(row_w, BLOCK, jnp.where(r == 31, tail[...], after), row_upper)
    put_mirror(row_z, 0, jnp.where(r == 0, tail[...], mirror_after), row_upper)
    put_mirror(row_z, BLOCK, mirror, row_upper)

    odd = [jnp.concatenate([pieces[2 * i + j, :16, :] for i in range(8)], axis=0) for j in range(2)]
    even = [jnp.concatenate([pieces[16 + 4 * i + j] for i in range(4)], axis=0) for j in range(4)]
    col_upper = c < 8
    put_window(col_w, 0, even[0], col_upper)
    put_window(col_w, BLOCK, odd[0], col_upper)
    put_window(col_w, 2 * BLOCK, jnp.where(c == 15, tail[...], even[2]), col_upper)
    put_mirror(col_z, 0, jnp.where(c == 0, tail[...], even[3]), col_upper)
    put_mirror(col_z, BLOCK, odd[1], col_upper)
    put_mirror(col_z, 2 * BLOCK, even[1], col_upper)

    acc[...] = jnp.zeros(acc.shape, jnp.float32)

    def step(at, carry):
        left, right = [], []
        for u in range(3 * GROUP):
            o = offsets[at * GROUP + u // 3, u % 3]
            for plane in range(2):
                left.append(
                    (row_w[plane, pl.ds(o, BLOCK), :] + row_z[plane, pl.ds(BLOCK - o, BLOCK), :])
                    .astype(jnp.bfloat16)
                )
                right.append(
                    (col_w[plane, pl.ds(o, 2 * BLOCK), :] + col_z[plane, pl.ds(BLOCK - o, 2 * BLOCK), :])
                    .astype(jnp.bfloat16)
                )
        acc[...] += dot_nt(jnp.concatenate(left, axis=1), jnp.concatenate(right, axis=1))
        return carry

    step(0, 0)
    block = acc[...] * (1.0 / (SNAPS * SHIFTS))
    cov[...] = block
    cov_near[...] = block
    image = dot_nn(basis[...], block, HIGH)
    for p in range(32):
        mapped[p] = image[4 * (p // 2) : 4 * (p // 2) + 4, SNAPS * (p % 2) : SNAPS * (p % 2) + SNAPS]


def covariance_block(place, offsets, own, mine, other, tail, pieces, basis):
    vmem = pl.BlockSpec(memory_space=pltpu.VMEM)
    return pl.pallas_call(
        covariance_kernel,
        name="covariance_block",
        in_specs=[pl.BlockSpec(memory_space=pltpu.SMEM)] * 2 + [vmem] * 6,
        out_specs=[vmem] * 3,
        out_shape=[
            jax.ShapeDtypeStruct((BLOCK, 2 * BLOCK), jnp.float32),
            pltpu.VMEM((BLOCK, 2 * BLOCK), jnp.float32),
            pltpu.VMEM((32, 4, SNAPS), jnp.float32),
        ],
        scratch_shapes=[
            pltpu.VMEM((2, 2 * BLOCK, SNAPS), jnp.float32),
            pltpu.VMEM((2, 2 * BLOCK, SNAPS), jnp.float32),
            pltpu.VMEM((2, 3 * BLOCK, SNAPS), jnp.float32),
            pltpu.VMEM((2, 3 * BLOCK, SNAPS), jnp.float32),
            pltpu.VMEM((BLOCK, 2 * BLOCK), jnp.float32),
        ],
    )(place, offsets, *[near(x) for x in (own, mine, other, tail, pieces, basis)])


def inverse_factor(gram):
    row_at = lax.broadcasted_iota(jnp.int32, (8, 2 * K), 0)
    lane_at = lax.broadcasted_iota(jnp.int32, (8, 2 * K), 1)
    tiles, done = [], []
    for t in range(K // 8):
        part = gram[8 * t : 8 * t + 8]
        eye = (lane_at == row_at + (K + 8 * t)).astype(jnp.float32)
        tiles.append(jnp.where(lane_at < K, jnp.concatenate([part, part], axis=1), eye))
        done.append(jnp.zeros((8, 2 * K), jnp.float32))
    for at in range(K // 8):
        own, rest = at, range(at + 1, K // 8)
        cols = [
            [jnp.broadcast_to(tiles[t][:, j : j + 1], (8, 2 * K)) for t in range(at, K // 8)]
            for j in range(8 * at, 8 * at + 8)
        ]
        for s in range(8):
            col = cols[s]
            below = row_at > s
            pivot = col[0][s : s + 1, :]
            inverse = 1.0 / pivot
            row = tiles[own][s : s + 1, :]
            scaled = row * inverse
            done[own] = jnp.where(row_at == s, row / jnp.sqrt(pivot), done[own])
            for k in range(s + 1, 8):
                share = cols[k][0][s : s + 1, :] * inverse
                left = [c - f * share for c, f in zip(cols[k], col)]
                left[0] = jnp.where(below, left[0], cols[k][0])
                cols[k] = left
            tiles[own] = jnp.where(below, tiles[own] - col[0] * scaled, tiles[own])
            for t in rest:
                tiles[t] = tiles[t] - col[t - at] * scaled
    return jnp.concatenate(done, axis=0)[:, K:]


def image_kernel(place, mapped, cov, kept, sent):
    image = jnp.concatenate(
        [jnp.concatenate([mapped[2 * i], mapped[2 * i + 1]], axis=1) for i in range(16)], axis=0
    )
    product = dot_nt(image, cov[...], HIGH)
    gram = dot_nt(image, image, HIGH)
    terms = jnp.concatenate([product, halves_side_by_side(gram)], axis=0)
    half = terms.shape[0] // 2
    first = place[1] % 2 == 0
    kept[...] = jnp.where(first, terms[:half], terms[half:])
    sent[...] = jnp.where(first, terms[half:], terms[:half])


def halves_side_by_side(gram):
    return jnp.concatenate([gram[: K // 2], gram[K // 2 :]], axis=1)


def halves_stacked(packed):
    return jnp.concatenate([packed[:, :K], packed[:, K:]], axis=0)


def first_factor_kernel(place, mine, other, mapped, grams):
    first = place[1] % 2 == 0
    total = jnp.concatenate(
        [jnp.where(first, mine[...], other[...]), jnp.where(first, other[...], mine[...])], axis=0
    )
    image = dot_nn(inverse_factor(halves_stacked(total[K:])), total[:K], HIGH)
    mapped[...] = image
    part = halves_side_by_side(dot_nt(image, image, HIGH))
    for i in range(grams.shape[0]):
        grams[i] = part


def last_factor_kernel(grams, mapped, basis):
    total = jnp.sum(grams[...], axis=0)
    basis[...] = dot_nn(inverse_factor(halves_stacked(total)), mapped[...], HIGH)


def local_call(kernel, shapes, *operands, result=pltpu.VMEM):
    spaces = [pltpu.SMEM if x.dtype == jnp.int32 else pltpu.VMEM for x in operands]
    return pl.pallas_call(
        kernel,
        in_specs=[pl.BlockSpec(memory_space=space) for space in spaces],
        out_shape=[result(s, jnp.float32) for s in shapes],
    )(*[x if x.dtype == jnp.int32 else near(x) for x in operands])


def exchanged(tiles, axis):
    return lax.all_to_all(tiles, axis, split_axis=0, concat_axis=0, tiled=True)


def total_over(tiles, axis):
    return sent_to_all(exchanged(tiles, axis).sum(axis=0), axis)


def piece_routes():
    routes = []
    for b in range(32):
        for q in range(16):
            if b % 2:
                c = (b - 1) // 2 if q % 2 == 0 else (31 - b) // 2
                to = q
            else:
                c = (b // 2, (30 - b) // 2, (b // 2 - 1) % 16, (16 - b // 2) % 16)[q % 4]
                to = q + 16
            routes.append((b * 16 + q, to * 16 + c))
    return routes


def per_device(snapshots, tail_sensors, shift_offsets, start_basis):
    r = lax.axis_index(ROW)
    c = lax.axis_index(SHIFT)
    own = snapshots.reshape(BLOCK, 2 * SNAPS)
    tail = tail_sensors.reshape(BLOCK, 2 * SNAPS)
    offsets = jnp.zeros((16, 2 * SNAPS), jnp.bfloat16)
    offsets = lax.dynamic_update_slice(offsets, shift_offsets.astype(jnp.bfloat16)[None], (0, 0))
    odd_piece = jnp.concatenate([lax.dynamic_slice_in_dim(own, 16 * (c // 2), 16, 0), offsets], 0)
    even_piece = lax.dynamic_slice_in_dim(own, 32 * (c // 4), 32, 0)
    piece = jnp.where(r % 2 == 1, odd_piece, even_piece)
    piece = lax.ppermute(piece, EVERY, piece_routes())
    half = lax.dynamic_slice_in_dim(own, BLOCK // 2 * lax.axis_index("core"), BLOCK // 2, 0)
    after = lax.ppermute(half, ROW, [(i, (i - 1) % 32) for i in range(32)])
    mirror = lax.ppermute(half, ROW, [(i, 31 - i) for i in range(32)])
    mirror_after = lax.ppermute(half, ROW, [(i, (32 - i) % 32) for i in range(32)])
    pieces = sent_to_all(piece, ROW)
    mine = jnp.stack([after, mirror, mirror_after])
    other = lax.ppermute(mine, "core", CORES_SWAPPED)
    every_offset = pieces[:16, 16, :3].astype(jnp.int32)
    place = jnp.stack([r, c]).astype(jnp.int32)
    cov, cov_near, mapped = covariance_block(
        place, every_offset, own, mine, other, tail, pieces, start_basis
    )
    mapped = total_over(mapped, ROW)
    half = (3 * K // 4, BLOCK)
    kept, sent = local_call(image_kernel, [half, half], place, mapped, cov_near)
    mine = sent_to_all(kept + lax.ppermute(sent, "core", CORES_SWAPPED), "z").sum(axis=0)
    other = lax.ppermute(mine, "core", CORES_SWAPPED)
    mapped, grams = local_call(
        first_factor_kernel, [(K, BLOCK), (4, K // 2, 2 * K)], place, mine, other
    )
    grams = sent_to_all(exchanged(grams, "row_0").sum(axis=0), "row_1")
    (basis,) = local_call(last_factor_kernel, [(K, BLOCK)], grams, mapped, result=jax.ShapeDtypeStruct)
    return (cov, basis)


def solution(mesh):
    split = Mesh(mesh.devices.reshape(4, 8, 8, 2), EVERY)
    in_specs = (P(ROW, None, None), P(), P(SHIFT), P(None, ROW))
    out_specs = (P(ROW, SHIFT), P(None, ROW))
    return jax.shard_map(
        per_device, mesh=split, in_specs=in_specs, out_specs=out_specs, check_vma=False
    )
```

```python
import jax
import jax.numpy as jnp
from jax import lax
from jax.experimental import pallas as pl
from jax.experimental.pallas import tpu as pltpu
from jax.sharding import Mesh
from jax.sharding import PartitionSpec as P


K = 64
SNAPS = 128
SHIFTS = 48
BLOCK = 128
GROUP = 16
ROW = ("row_0", "row_1")
SHIFT = ("z", "core")
EVERY = (*ROW, *SHIFT)
HALF_ROOT = 0.7071067811865476
HIGH = lax.Precision.HIGHEST


def dot_nt(a, b, precision=None):
    return lax.dot_general(
        a, b, (((1,), (1,)), ((), ())), precision=precision, preferred_element_type=jnp.float32
    )


def dot_nn(a, b, precision=None):
    return lax.dot_general(
        a, b, (((1,), (0,)), ((), ())), precision=precision, preferred_element_type=jnp.float32
    )


def near(x):
    return pltpu.with_memory_space_constraint(x, pltpu.VMEM)


def sent_to_all(x, axis):
    copies = jnp.broadcast_to(x, (lax.axis_size(axis), *x.shape))
    return lax.all_to_all(copies, axis, split_axis=0, concat_axis=0, tiled=True)


def covariance_kernel(
    place, offsets, own, after, mirror, mirror_after, tail, pieces, basis,
    cov, cov_near, mapped, row_w, row_z, col_w, col_z, acc,
):
    r = place[0]
    c = place[1]
    flip = (
        lax.broadcasted_iota(jnp.int32, (BLOCK, BLOCK), 0)
        + lax.broadcasted_iota(jnp.int32, (BLOCK, BLOCK), 1)
        == BLOCK - 1
    ).astype(jnp.bfloat16)

    def put_window(ref, at, block, upper):
        re = block[:, :SNAPS].astype(jnp.float32) * HALF_ROOT
        im = block[:, SNAPS:].astype(jnp.float32) * HALF_ROOT
        ref[0, pl.ds(at, BLOCK), :] = jnp.where(upper, re, im)
        ref[1, pl.ds(at, BLOCK), :] = jnp.where(upper, im, -re)

    def put_mirror(ref, at, block, upper):
        turned = dot_nn(flip, block) * HALF_ROOT
        re = turned[:, :SNAPS]
        im = turned[:, SNAPS:]
        ref[0, pl.ds(at, BLOCK), :] = jnp.where(upper, re, -im)
        ref[1, pl.ds(at, BLOCK), :] = jnp.where(upper, im, re)

    row_upper = r < 16
    put_window(row_w, 0, own[...], row_upper)
    put_window(row_w, BLOCK, jnp.where(r == 31, tail[...], after[...]), row_upper)
    put_mirror(row_z, 0, jnp.where(r == 0, tail[...], mirror_after[...]), row_upper)
    put_mirror(row_z, BLOCK, mirror[...], row_upper)

    odd = [jnp.concatenate([pieces[2 * i + j, :16, :] for i in range(8)], axis=0) for j in range(2)]
    even = [jnp.concatenate([pieces[16 + 4 * i + j] for i in range(4)], axis=0) for j in range(4)]
    col_upper = c < 8
    put_window(col_w, 0, even[0], col_upper)
    put_window(col_w, BLOCK, odd[0], col_upper)
    put_window(col_w, 2 * BLOCK, jnp.where(c == 15, tail[...], even[2]), col_upper)
    put_mirror(col_z, 0, jnp.where(c == 0, tail[...], even[3]), col_upper)
    put_mirror(col_z, BLOCK, odd[1], col_upper)
    put_mirror(col_z, 2 * BLOCK, even[1], col_upper)

    acc[...] = jnp.zeros(acc.shape, jnp.float32)

    def step(at, carry):
        left, right = [], []
        for u in range(3 * GROUP):
            o = offsets[at * GROUP + u // 3, u % 3]
            for plane in range(2):
                left.append(
                    (row_w[plane, pl.ds(o, BLOCK), :] + row_z[plane, pl.ds(BLOCK - o, BLOCK), :])
                    .astype(jnp.bfloat16)
                )
                right.append(
                    (col_w[plane, pl.ds(o, 2 * BLOCK), :] + col_z[plane, pl.ds(BLOCK - o, 2 * BLOCK), :])
                    .astype(jnp.bfloat16)
                )
        acc[...] += dot_nt(jnp.concatenate(left, axis=1), jnp.concatenate(right, axis=1))
        return carry

    step(0, 0)
    block = acc[...] * (1.0 / (SNAPS * SHIFTS))
    cov[...] = block
    cov_near[...] = block
    image = dot_nn(basis[...], block, HIGH)
    for t in range(8):
        mapped[t] = image[8 * t : 8 * t + 8]


def covariance_block(place, offsets, own, after, mirror, mirror_after, tail, pieces, basis):
    vmem = pl.BlockSpec(memory_space=pltpu.VMEM)
    return pl.pallas_call(
        covariance_kernel,
        name="covariance_block",
        in_specs=[pl.BlockSpec(memory_space=pltpu.SMEM)] * 2 + [vmem] * 7,
        out_specs=[vmem] * 3,
        out_shape=[
            jax.ShapeDtypeStruct((BLOCK, 2 * BLOCK), jnp.float32),
            pltpu.VMEM((BLOCK, 2 * BLOCK), jnp.float32),
            pltpu.VMEM((8, 8, 2 * BLOCK), jnp.float32),
        ],
        scratch_shapes=[
            pltpu.VMEM((2, 2 * BLOCK, SNAPS), jnp.float32),
            pltpu.VMEM((2, 2 * BLOCK, SNAPS), jnp.float32),
            pltpu.VMEM((2, 3 * BLOCK, SNAPS), jnp.float32),
            pltpu.VMEM((2, 3 * BLOCK, SNAPS), jnp.float32),
            pltpu.VMEM((BLOCK, 2 * BLOCK), jnp.float32),
        ],
    )(place, offsets, *[near(x) for x in (own, after, mirror, mirror_after, tail, pieces, basis)])


def inverse_factor(gram):
    row_at = lax.broadcasted_iota(jnp.int32, (8, 2 * K), 0)
    lane_at = lax.broadcasted_iota(jnp.int32, (8, 2 * K), 1)
    tiles, done = [], []
    for t in range(K // 8):
        part = gram[8 * t : 8 * t + 8]
        eye = (lane_at == row_at + (K + 8 * t)).astype(jnp.float32)
        tiles.append(jnp.where(lane_at < K, jnp.concatenate([part, part], axis=1), eye))
        done.append(jnp.zeros((8, 2 * K), jnp.float32))
    for at in range(K // 8):
        own, rest = at, range(at + 1, K // 8)
        cols = [
            [jnp.broadcast_to(tiles[t][:, j : j + 1], (8, 2 * K)) for t in range(at, K // 8)]
            for j in range(8 * at, 8 * at + 8)
        ]
        for s in range(8):
            col = cols[s]
            below = row_at > s
            pivot = col[0][s : s + 1, :]
            inverse = 1.0 / pivot
            row = tiles[own][s : s + 1, :]
            scaled = row * inverse
            done[own] = jnp.where(row_at == s, row / jnp.sqrt(pivot), done[own])
            for k in range(s + 1, 8):
                share = cols[k][0][s : s + 1, :] * inverse
                left = [c - f * share for c, f in zip(cols[k], col)]
                left[0] = jnp.where(below, left[0], cols[k][0])
                cols[k] = left
            tiles[own] = jnp.where(below, tiles[own] - col[0] * scaled, tiles[own])
            for t in rest:
                tiles[t] = tiles[t] - col[t - at] * scaled
    return jnp.concatenate(done, axis=0)[:, K:]


def image_kernel(place, mapped, cov, kept, sent):
    image = jnp.concatenate([mapped[t] for t in range(8)], axis=0)
    product = dot_nt(image, cov[...], HIGH)
    gram = dot_nt(image, image, HIGH)
    terms = jnp.concatenate([product, halves_side_by_side(gram)], axis=0)
    half = terms.shape[0] // 2
    first = place[1] % 2 == 0
    kept[...] = jnp.where(first, terms[:half], terms[half:])
    sent[...] = jnp.where(first, terms[half:], terms[:half])


def halves_side_by_side(gram):
    return jnp.concatenate([gram[: K // 2], gram[K // 2 :]], axis=1)


def distinct_blocks(gram):
    h = K // 2
    wide = jnp.concatenate([gram[:h, :h], gram[h:, :h], gram[h:, h:]], axis=1)
    return jnp.concatenate(
        [
            jnp.concatenate([wide[8 * i : 8 * i + 8], wide[24:, h * i : h * i + h]], axis=1)
            for i in range(3)
        ],
        axis=0,
    )


def from_distinct_blocks(packed):
    h = K // 2
    last = jnp.concatenate([packed[8 * i : 8 * i + 8, 3 * h :] for i in range(3)], axis=1)
    wide = jnp.concatenate([packed[:, : 3 * h], last], axis=0)
    low = wide[:, h : 2 * h]
    top = jnp.concatenate([wide[:, :h], low.T], axis=1)
    return jnp.concatenate([top, jnp.concatenate([low, wide[:, 2 * h :]], axis=1)], axis=0)


def halves_stacked(packed):
    return jnp.concatenate([packed[:, :K], packed[:, K:]], axis=0)


def first_factor_kernel(place, mine, other, mapped, grams):
    first = place[1] % 2 == 0
    total = jnp.concatenate(
        [jnp.where(first, mine[...], other[...]), jnp.where(first, other[...], mine[...])], axis=0
    )
    image = dot_nn(inverse_factor(halves_stacked(total[K:])), total[:K], HIGH)
    mapped[...] = image
    part = distinct_blocks(dot_nt(image, image, HIGH))
    for i in range(grams.shape[0]):
        grams[i] = part


def last_factor_kernel(grams, mapped, basis):
    total = jnp.sum(grams[...], axis=0)
    basis[...] = dot_nn(inverse_factor(from_distinct_blocks(total)), mapped[...], HIGH)


def local_call(kernel, shapes, *operands, result=pltpu.VMEM):
    spaces = [pltpu.SMEM if x.dtype == jnp.int32 else pltpu.VMEM for x in operands]
    return pl.pallas_call(
        kernel,
        in_specs=[pl.BlockSpec(memory_space=space) for space in spaces],
        out_shape=[result(s, jnp.float32) for s in shapes],
    )(*[x if x.dtype == jnp.int32 else near(x) for x in operands])


def exchanged(tiles, axis):
    return lax.all_to_all(tiles, axis, split_axis=0, concat_axis=0, tiled=True)


def piece_routes():
    routes = []
    for b in range(32):
        for q in range(16):
            if b % 2:
                c = (b - 1) // 2 if q % 2 == 0 else (31 - b) // 2
                to = q
            else:
                c = (b // 2, (30 - b) // 2, (b // 2 - 1) % 16, (16 - b // 2) % 16)[q % 4]
                to = q + 16
            routes.append((b * 16 + q, to * 16 + c))
    return routes


def per_device(snapshots, tail_sensors, shift_offsets, start_basis):
    r = lax.axis_index(ROW)
    c = lax.axis_index(SHIFT)
    own = snapshots.reshape(BLOCK, 2 * SNAPS)
    tail = tail_sensors.reshape(BLOCK, 2 * SNAPS)
    offsets = jnp.zeros((16, 2 * SNAPS), jnp.bfloat16)
    offsets = lax.dynamic_update_slice(offsets, shift_offsets.astype(jnp.bfloat16)[None], (0, 0))
    odd_piece = jnp.concatenate([lax.dynamic_slice_in_dim(own, 16 * (c // 2), 16, 0), offsets], 0)
    even_piece = lax.dynamic_slice_in_dim(own, 32 * (c // 4), 32, 0)
    piece = jnp.where(r % 2 == 1, odd_piece, even_piece)
    piece = lax.ppermute(piece, EVERY, piece_routes())
    after = lax.ppermute(own, ROW, [(i, (i - 1) % 32) for i in range(32)])
    mirror = lax.ppermute(own, ROW, [(i, 31 - i) for i in range(32)])
    mirror_after = lax.ppermute(own, ROW, [(i, (32 - i) % 32) for i in range(32)])
    pieces = sent_to_all(piece, ROW)
    every_offset = pieces[:16, 16, :3].astype(jnp.int32)
    place = jnp.stack([r, c]).astype(jnp.int32)
    cov, cov_near, mapped = covariance_block(
        place, every_offset, own, after, mirror, mirror_after, tail, pieces, start_basis
    )
    mapped = exchanged(mapped, "row_1").sum(axis=0)
    mapped = sent_to_all(sent_to_all(mapped, "row_0").sum(axis=0), "row_1")
    half = (3 * K // 4, BLOCK)
    kept, sent = local_call(image_kernel, [half, half], place, mapped, cov_near)
    swap = [(0, 1), (1, 0)]
    mine = sent_to_all(kept + lax.ppermute(sent, "core", swap), "z").sum(axis=0)
    other = lax.ppermute(mine, "core", swap)
    mapped, grams = local_call(
        first_factor_kernel, [(K, BLOCK), (4, 3 * K // 8, 2 * K)], place, mine, other
    )
    grams = sent_to_all(exchanged(grams, "row_0").sum(axis=0), "row_1")
    (basis,) = local_call(last_factor_kernel, [(K, BLOCK)], grams, mapped, result=jax.ShapeDtypeStruct)
    return (cov, basis)


def solution(mesh):
    split = Mesh(mesh.devices.reshape(4, 8, 8, 2), EVERY)
    in_specs = (P(ROW, None, None), P(), P(SHIFT), P(None, ROW))
    out_specs = (P(ROW, SHIFT), P(None, ROW))
    return jax.shard_map(
        per_device, mesh=split, in_specs=in_specs, out_specs=out_specs, check_vma=False
    )
```

```python
import jax
import jax.numpy as jnp
from jax import lax
from jax.experimental import pallas as pl
from jax.experimental.pallas import tpu as pltpu
from jax.sharding import Mesh
from jax.sharding import PartitionSpec as P


K = 64
SNAPS = 128
SHIFTS = 48
BLOCK = 128
GROUP = 16
ROW = ("row_0", "row_1")
SHIFT = ("z", "core")
EVERY = (*ROW, *SHIFT)
HALF_ROOT = 0.7071067811865476
HIGH = lax.Precision.HIGHEST


def dot_nt(a, b, precision=None):
    return lax.dot_general(
        a, b, (((1,), (1,)), ((), ())), precision=precision, preferred_element_type=jnp.float32
    )


def dot_nn(a, b, precision=None):
    return lax.dot_general(
        a, b, (((1,), (0,)), ((), ())), precision=precision, preferred_element_type=jnp.float32
    )


def near(x):
    return pltpu.with_memory_space_constraint(x, pltpu.VMEM)


def sent_to_all(x, axis):
    copies = jnp.broadcast_to(x, (lax.axis_size(axis), *x.shape))
    return lax.all_to_all(copies, axis, split_axis=0, concat_axis=0, tiled=True)


def covariance_kernel(
    place, offsets, own, after, mirror, mirror_after, tail, pieces, basis,
    cov, cov_near, mapped, row_w, row_z, col_w, col_z, acc,
):
    r = place[0]
    c = place[1]
    flip = (
        lax.broadcasted_iota(jnp.int32, (BLOCK, BLOCK), 0)
        + lax.broadcasted_iota(jnp.int32, (BLOCK, BLOCK), 1)
        == BLOCK - 1
    ).astype(jnp.bfloat16)

    def put_window(ref, at, block, upper):
        re = block[:, :SNAPS].astype(jnp.float32) * HALF_ROOT
        im = block[:, SNAPS:].astype(jnp.float32) * HALF_ROOT
        ref[0, pl.ds(at, BLOCK), :] = jnp.where(upper, re, im)
        ref[1, pl.ds(at, BLOCK), :] = jnp.where(upper, im, -re)

    def put_mirror(ref, at, block, upper):
        turned = dot_nn(flip, block) * HALF_ROOT
        re = turned[:, :SNAPS]
        im = turned[:, SNAPS:]
        ref[0, pl.ds(at, BLOCK), :] = jnp.where(upper, re, -im)
        ref[1, pl.ds(at, BLOCK), :] = jnp.where(upper, im, re)

    row_upper = r < 16
    put_window(row_w, 0, own[...], row_upper)
    put_window(row_w, BLOCK, jnp.where(r == 31, tail[...], after[...]), row_upper)
    put_mirror(row_z, 0, jnp.where(r == 0, tail[...], mirror_after[...]), row_upper)
    put_mirror(row_z, BLOCK, mirror[...], row_upper)

    odd = [jnp.concatenate([pieces[2 * i + j, :16, :] for i in range(8)], axis=0) for j in range(2)]
    even = [jnp.concatenate([pieces[16 + 4 * i + j] for i in range(4)], axis=0) for j in range(4)]
    col_upper = c < 8
    put_window(col_w, 0, even[0], col_upper)
    put_window(col_w, BLOCK, odd[0], col_upper)
    put_window(col_w, 2 * BLOCK, jnp.where(c == 15, tail[...], even[2]), col_upper)
    put_mirror(col_z, 0, jnp.where(c == 0, tail[...], even[3]), col_upper)
    put_mirror(col_z, BLOCK, odd[1], col_upper)
    put_mirror(col_z, 2 * BLOCK, even[1], col_upper)

    acc[...] = jnp.zeros(acc.shape, jnp.float32)

    def step(at, carry):
        left, right = [], []
        for u in range(3 * GROUP):
            o = offsets[at * GROUP + u // 3, u % 3]
            for plane in range(2):
                left.append(
                    (row_w[plane, pl.ds(o, BLOCK), :] + row_z[plane, pl.ds(BLOCK - o, BLOCK), :])
                    .astype(jnp.bfloat16)
                )
                right.append(
                    (col_w[plane, pl.ds(o, 2 * BLOCK), :] + col_z[plane, pl.ds(BLOCK - o, 2 * BLOCK), :])
                    .astype(jnp.bfloat16)
                )
        acc[...] += dot_nt(jnp.concatenate(left, axis=1), jnp.concatenate(right, axis=1))
        return carry

    step(0, 0)
    block = acc[...] * (1.0 / (SNAPS * SHIFTS))
    cov[...] = block
    cov_near[...] = block
    image = dot_nn(basis[...], block, HIGH)
    for p in range(32):
        mapped[p] = image[4 * (p // 2) : 4 * (p // 2) + 4, SNAPS * (p % 2) : SNAPS * (p % 2) + SNAPS]


def covariance_block(place, offsets, own, after, mirror, mirror_after, tail, pieces, basis):
    vmem = pl.BlockSpec(memory_space=pltpu.VMEM)
    return pl.pallas_call(
        covariance_kernel,
        name="covariance_block",
        in_specs=[pl.BlockSpec(memory_space=pltpu.SMEM)] * 2 + [vmem] * 7,
        out_specs=[vmem] * 3,
        out_shape=[
            jax.ShapeDtypeStruct((BLOCK, 2 * BLOCK), jnp.float32),
            pltpu.VMEM((BLOCK, 2 * BLOCK), jnp.float32),
            pltpu.VMEM((32, 4, SNAPS), jnp.float32),
        ],
        scratch_shapes=[
            pltpu.VMEM((2, 2 * BLOCK, SNAPS), jnp.float32),
            pltpu.VMEM((2, 2 * BLOCK, SNAPS), jnp.float32),
            pltpu.VMEM((2, 3 * BLOCK, SNAPS), jnp.float32),
            pltpu.VMEM((2, 3 * BLOCK, SNAPS), jnp.float32),
            pltpu.VMEM((BLOCK, 2 * BLOCK), jnp.float32),
        ],
    )(place, offsets, *[near(x) for x in (own, after, mirror, mirror_after, tail, pieces, basis)])


def inverse_factor(gram):
    row_at = lax.broadcasted_iota(jnp.int32, (8, 2 * K), 0)
    lane_at = lax.broadcasted_iota(jnp.int32, (8, 2 * K), 1)
    tiles, done = [], []
    for t in range(K // 8):
        part = gram[8 * t : 8 * t + 8]
        eye = (lane_at == row_at + (K + 8 * t)).astype(jnp.float32)
        tiles.append(jnp.where(lane_at < K, jnp.concatenate([part, part], axis=1), eye))
        done.append(jnp.zeros((8, 2 * K), jnp.float32))
    for at in range(K // 8):
        own, rest = at, range(at + 1, K // 8)
        cols = [
            [jnp.broadcast_to(tiles[t][:, j : j + 1], (8, 2 * K)) for t in range(at, K // 8)]
            for j in range(8 * at, 8 * at + 8)
        ]
        for s in range(8):
            col = cols[s]
            below = row_at > s
            pivot = col[0][s : s + 1, :]
            inverse = 1.0 / pivot
            row = tiles[own][s : s + 1, :]
            scaled = row * inverse
            done[own] = jnp.where(row_at == s, row / jnp.sqrt(pivot), done[own])
            for k in range(s + 1, 8):
                share = cols[k][0][s : s + 1, :] * inverse
                left = [c - f * share for c, f in zip(cols[k], col)]
                left[0] = jnp.where(below, left[0], cols[k][0])
                cols[k] = left
            tiles[own] = jnp.where(below, tiles[own] - col[0] * scaled, tiles[own])
            for t in rest:
                tiles[t] = tiles[t] - col[t - at] * scaled
    return jnp.concatenate(done, axis=0)[:, K:]


def image_kernel(mapped, cov, terms):
    image = jnp.concatenate(
        [jnp.concatenate([mapped[2 * i], mapped[2 * i + 1]], axis=1) for i in range(16)], axis=0
    )
    terms[:K] = dot_nt(image, cov[...], HIGH)
    terms[K:] = halves_side_by_side(dot_nt(image, image, HIGH))


def halves_side_by_side(gram):
    return jnp.concatenate([gram[: K // 2], gram[K // 2 :]], axis=1)


def halves_stacked(packed):
    return jnp.concatenate([packed[:, :K], packed[:, K:]], axis=0)


def first_factor_kernel(total, mapped, grams):
    image = dot_nn(inverse_factor(halves_stacked(total[K:])), total[:K], HIGH)
    mapped[...] = image
    part = halves_side_by_side(dot_nt(image, image, HIGH))
    for i in range(grams.shape[0]):
        grams[i] = part


def last_factor_kernel(grams, mapped, basis):
    total = jnp.sum(grams[...], axis=0)
    basis[...] = dot_nn(inverse_factor(halves_stacked(total)), mapped[...], HIGH)


def local_call(kernel, shapes, *operands, result=pltpu.VMEM):
    spaces = [pltpu.SMEM if x.dtype == jnp.int32 else pltpu.VMEM for x in operands]
    return pl.pallas_call(
        kernel,
        in_specs=[pl.BlockSpec(memory_space=space) for space in spaces],
        out_shape=[result(s, jnp.float32) for s in shapes],
    )(*[x if x.dtype == jnp.int32 else near(x) for x in operands])


def exchanged(tiles, axis):
    return lax.all_to_all(tiles, axis, split_axis=0, concat_axis=0, tiled=True)


def total_over(tiles, axis):
    return sent_to_all(exchanged(tiles, axis).sum(axis=0), axis)


def piece_routes():
    routes = []
    for b in range(32):
        for q in range(16):
            if b % 2:
                c = (b - 1) // 2 if q % 2 == 0 else (31 - b) // 2
                to = q
            else:
                c = (b // 2, (30 - b) // 2, (b // 2 - 1) % 16, (16 - b // 2) % 16)[q % 4]
                to = q + 16
            routes.append((b * 16 + q, to * 16 + c))
    return routes


def per_device(snapshots, tail_sensors, shift_offsets, start_basis):
    r = lax.axis_index(ROW)
    c = lax.axis_index(SHIFT)
    own = snapshots.reshape(BLOCK, 2 * SNAPS)
    tail = tail_sensors.reshape(BLOCK, 2 * SNAPS)
    offsets = jnp.zeros((16, 2 * SNAPS), jnp.bfloat16)
    offsets = lax.dynamic_update_slice(offsets, shift_offsets.astype(jnp.bfloat16)[None], (0, 0))
    odd_piece = jnp.concatenate([lax.dynamic_slice_in_dim(own, 16 * (c // 2), 16, 0), offsets], 0)
    even_piece = lax.dynamic_slice_in_dim(own, 32 * (c // 4), 32, 0)
    piece = jnp.where(r % 2 == 1, odd_piece, even_piece)
    piece = lax.ppermute(piece, EVERY, piece_routes())
    after = lax.ppermute(own, ROW, [(i, (i - 1) % 32) for i in range(32)])
    mirror = lax.ppermute(own, ROW, [(i, 31 - i) for i in range(32)])
    mirror_after = lax.ppermute(own, ROW, [(i, (32 - i) % 32) for i in range(32)])
    pieces = sent_to_all(piece, ROW)
    every_offset = pieces[:16, 16, :3].astype(jnp.int32)
    place = jnp.stack([r, c]).astype(jnp.int32)
    cov, cov_near, mapped = covariance_block(
        place, every_offset, own, after, mirror, mirror_after, tail, pieces, start_basis
    )
    mapped = total_over(mapped, ROW)
    (terms,) = local_call(image_kernel, [(3 * K // 2, BLOCK)], mapped, cov_near)
    both = lax.all_gather(terms.reshape(2, 3 * K // 4, BLOCK), "core")
    mine = lax.dynamic_index_in_dim(both, lax.axis_index("core"), 1, keepdims=False).sum(axis=0)
    mine = sent_to_all(mine, "z").sum(axis=0)
    total = lax.all_gather(mine, "core", tiled=True)
    mapped, grams = local_call(first_factor_kernel, [(K, BLOCK), (4, K // 2, 2 * K)], total)
    grams = sent_to_all(exchanged(grams, "row_0").sum(axis=0), "row_1")
    (basis,) = local_call(last_factor_kernel, [(K, BLOCK)], grams, mapped, result=jax.ShapeDtypeStruct)
    return (cov, basis)


def solution(mesh):
    split = Mesh(mesh.devices.reshape(4, 8, 8, 2), EVERY)
    in_specs = (P(ROW, None, None), P(), P(SHIFT), P(None, ROW))
    out_specs = (P(ROW, SHIFT), P(None, ROW))
    return jax.shard_map(
        per_device, mesh=split, in_specs=in_specs, out_specs=out_specs, check_vma=False
    )
```

```python
import jax
import jax.numpy as jnp
from jax import lax
from jax.experimental import pallas as pl
from jax.experimental.pallas import tpu as pltpu
from jax.sharding import Mesh
from jax.sharding import PartitionSpec as P


K = 64
SNAPS = 128
SHIFTS = 48
BLOCK = 128
GROUP = 16
ROW = ("row_0", "row_1")
SHIFT = ("z", "core")
EVERY = (*ROW, *SHIFT)
HALF_ROOT = 0.7071067811865476
HIGH = lax.Precision.HIGHEST


def dot_nt(a, b, precision=None):
    return lax.dot_general(
        a, b, (((1,), (1,)), ((), ())), precision=precision, preferred_element_type=jnp.float32
    )


def dot_nn(a, b, precision=None):
    return lax.dot_general(
        a, b, (((1,), (0,)), ((), ())), precision=precision, preferred_element_type=jnp.float32
    )


def near(x):
    return pltpu.with_memory_space_constraint(x, pltpu.VMEM)


def sent_to_all(x, axis):
    copies = jnp.broadcast_to(x, (lax.axis_size(axis), *x.shape))
    return lax.all_to_all(copies, axis, split_axis=0, concat_axis=0, tiled=True)


def covariance_kernel(
    own, after, mirror, mirror_after, tail, pieces, basis,
    cov, cov_near, mapped, row_w, row_z, col_w, col_z, acc,
):
    r = lax.axis_index(ROW)
    c = lax.axis_index(SHIFT)
    offsets = []
    for q in range(16):
        held = pieces[q, 16:, :SNAPS].astype(jnp.float32).astype(jnp.int32)
        offsets += [held[i, 0] for i in range(3)]
    flip = (
        lax.broadcasted_iota(jnp.int32, (BLOCK, BLOCK), 0)
        + lax.broadcasted_iota(jnp.int32, (BLOCK, BLOCK), 1)
        == BLOCK - 1
    ).astype(jnp.bfloat16)

    def put_window(ref, at, block, upper):
        re = block[:, :SNAPS].astype(jnp.float32) * HALF_ROOT
        im = block[:, SNAPS:].astype(jnp.float32) * HALF_ROOT
        ref[0, pl.ds(at, BLOCK), :] = jnp.where(upper, re, im)
        ref[1, pl.ds(at, BLOCK), :] = jnp.where(upper, im, -re)

    def put_mirror(ref, at, block, upper):
        turned = dot_nn(flip, block) * HALF_ROOT
        re = turned[:, :SNAPS]
        im = turned[:, SNAPS:]
        ref[0, pl.ds(at, BLOCK), :] = jnp.where(upper, re, -im)
        ref[1, pl.ds(at, BLOCK), :] = jnp.where(upper, im, re)

    row_upper = r < 16
    put_window(row_w, 0, own[...], row_upper)
    put_window(row_w, BLOCK, jnp.where(r == 31, tail[...], after[...]), row_upper)
    put_mirror(row_z, 0, jnp.where(r == 0, tail[...], mirror_after[...]), row_upper)
    put_mirror(row_z, BLOCK, mirror[...], row_upper)

    odd = [jnp.concatenate([pieces[2 * i + j, :16, :] for i in range(8)], axis=0) for j in range(2)]
    even = [jnp.concatenate([pieces[16 + 4 * i + j] for i in range(4)], axis=0) for j in range(4)]
    col_upper = c < 8
    put_window(col_w, 0, even[0], col_upper)
    put_window(col_w, BLOCK, odd[0], col_upper)
    put_window(col_w, 2 * BLOCK, jnp.where(c == 15, tail[...], even[2]), col_upper)
    put_mirror(col_z, 0, jnp.where(c == 0, tail[...], even[3]), col_upper)
    put_mirror(col_z, BLOCK, odd[1], col_upper)
    put_mirror(col_z, 2 * BLOCK, even[1], col_upper)

    acc[...] = jnp.zeros(acc.shape, jnp.float32)

    def step(carry):
        left, right = [], []
        for u in range(3 * GROUP):
            o = offsets[u]
            for plane in range(2):
                left.append(
                    (row_w[plane, pl.ds(o, BLOCK), :] + row_z[plane, pl.ds(BLOCK - o, BLOCK), :])
                    .astype(jnp.bfloat16)
                )
                right.append(
                    (col_w[plane, pl.ds(o, 2 * BLOCK), :] + col_z[plane, pl.ds(BLOCK - o, 2 * BLOCK), :])
                    .astype(jnp.bfloat16)
                )
        acc[...] += dot_nt(jnp.concatenate(left, axis=1), jnp.concatenate(right, axis=1))
        return carry

    step(0)
    block = acc[...] * (1.0 / (SNAPS * SHIFTS))
    cov[...] = block
    cov_near[...] = block
    image = dot_nn(basis[...], block, HIGH)
    for p in range(32):
        mapped[p] = image[4 * (p // 2) : 4 * (p // 2) + 4, SNAPS * (p % 2) : SNAPS * (p % 2) + SNAPS]


def covariance_block(own, after, mirror, mirror_after, tail, pieces, basis):
    vmem = pl.BlockSpec(memory_space=pltpu.VMEM)
    return pl.pallas_call(
        covariance_kernel,
        name="covariance_block",
        in_specs=[vmem] * 7,
        out_specs=[vmem] * 3,
        out_shape=[
            jax.ShapeDtypeStruct((BLOCK, 2 * BLOCK), jnp.float32),
            pltpu.VMEM((BLOCK, 2 * BLOCK), jnp.float32),
            pltpu.VMEM((32, 4, SNAPS), jnp.float32),
        ],
        scratch_shapes=[
            pltpu.VMEM((2, 2 * BLOCK, SNAPS), jnp.float32),
            pltpu.VMEM((2, 2 * BLOCK, SNAPS), jnp.float32),
            pltpu.VMEM((2, 3 * BLOCK, SNAPS), jnp.float32),
            pltpu.VMEM((2, 3 * BLOCK, SNAPS), jnp.float32),
            pltpu.VMEM((BLOCK, 2 * BLOCK), jnp.float32),
        ],
    )(*[near(x) for x in (own, after, mirror, mirror_after, tail, pieces, basis)])


def inverse_factor(gram):
    row_at = lax.broadcasted_iota(jnp.int32, (8, 2 * K), 0)
    lane_at = lax.broadcasted_iota(jnp.int32, (8, 2 * K), 1)
    tiles, done = [], []
    for t in range(K // 8):
        part = gram[8 * t : 8 * t + 8]
        eye = (lane_at == row_at + (K + 8 * t)).astype(jnp.float32)
        tiles.append(jnp.where(lane_at < K, jnp.concatenate([part, part], axis=1), eye))
        done.append(jnp.zeros((8, 2 * K), jnp.float32))
    for at in range(K // 8):
        own, rest = at, range(at + 1, K // 8)
        cols = [
            [jnp.broadcast_to(tiles[t][:, j : j + 1], (8, 2 * K)) for t in range(at, K // 8)]
            for j in range(8 * at, 8 * at + 8)
        ]
        for s in range(8):
            col = cols[s]
            below = row_at > s
            pivot = col[0][s : s + 1, :]
            inverse = 1.0 / pivot
            row = tiles[own][s : s + 1, :]
            scaled = row * inverse
            done[own] = jnp.where(row_at == s, row / jnp.sqrt(pivot), done[own])
            for k in range(s + 1, 8):
                share = cols[k][0][s : s + 1, :] * inverse
                left = [c - f * share for c, f in zip(cols[k], col)]
                left[0] = jnp.where(below, left[0], cols[k][0])
                cols[k] = left
            tiles[own] = jnp.where(below, tiles[own] - col[0] * scaled, tiles[own])
            for t in rest:
                tiles[t] = tiles[t] - col[t - at] * scaled
    return jnp.concatenate(done, axis=0)[:, K:]


def image_kernel(mapped, cov, terms):
    image = jnp.concatenate(
        [jnp.concatenate([mapped[2 * i], mapped[2 * i + 1]], axis=1) for i in range(16)], axis=0
    )
    terms[:K] = dot_nt(image, cov[...], HIGH)
    terms[K:] = halves_side_by_side(dot_nt(image, image, HIGH))


def halves_side_by_side(gram):
    return jnp.concatenate([gram[: K // 2], gram[K // 2 :]], axis=1)


def halves_stacked(packed):
    return jnp.concatenate([packed[:, :K], packed[:, K:]], axis=0)


def first_factor_kernel(total, mapped, grams):
    image = dot_nn(inverse_factor(halves_stacked(total[K:])), total[:K], HIGH)
    mapped[...] = image
    part = halves_side_by_side(dot_nt(image, image, HIGH))
    for i in range(grams.shape[0]):
        grams[i] = part


def last_factor_kernel(grams, mapped, basis):
    total = jnp.sum(grams[...], axis=0)
    basis[...] = dot_nn(inverse_factor(halves_stacked(total)), mapped[...], HIGH)


def local_call(kernel, shapes, *operands, result=pltpu.VMEM):
    spaces = [pltpu.SMEM if x.dtype == jnp.int32 else pltpu.VMEM for x in operands]
    return pl.pallas_call(
        kernel,
        in_specs=[pl.BlockSpec(memory_space=space) for space in spaces],
        out_shape=[result(s, jnp.float32) for s in shapes],
    )(*[x if x.dtype == jnp.int32 else near(x) for x in operands])


def exchanged(tiles, axis):
    return lax.all_to_all(tiles, axis, split_axis=0, concat_axis=0, tiled=True)


def total_over(tiles, axis):
    return sent_to_all(exchanged(tiles, axis).sum(axis=0), axis)


def piece_routes():
    routes = []
    for b in range(32):
        for q in range(16):
            if b % 2:
                c = (b - 1) // 2 if q % 2 == 0 else (31 - b) // 2
                to = q
            else:
                c = (b // 2, (30 - b) // 2, (b // 2 - 1) % 16, (16 - b // 2) % 16)[q % 4]
                to = q + 16
            routes.append((b * 16 + q, to * 16 + c))
    return routes


def per_device(snapshots, tail_sensors, shift_offsets, start_basis):
    r = lax.axis_index(ROW)
    c = lax.axis_index(SHIFT)
    tail = tail_sensors.reshape(BLOCK, 2 * SNAPS)
    offsets = jnp.zeros((16, 2 * SNAPS), jnp.bfloat16)
    offsets = lax.dynamic_update_slice(offsets, shift_offsets.astype(jnp.bfloat16)[:, None], (0, 0))
    core = lax.axis_index("core").astype(jnp.uint32)
    own, core, offsets = lax.optimization_barrier((snapshots, core, offsets))
    own = own.reshape(BLOCK, 2 * SNAPS)
    odd_piece = jnp.concatenate([lax.dynamic_slice_in_dim(own, 16 * (c // 2), 16, 0), offsets], 0)
    even_piece = lax.dynamic_slice_in_dim(own, 32 * (c // 4), 32, 0)
    piece = jnp.where(r % 2 == 1, odd_piece, even_piece)
    piece = lax.ppermute(piece, EVERY, piece_routes())
    after = lax.ppermute(own, ROW, [(i, (i - 1) % 32) for i in range(32)])
    mirror = lax.ppermute(own, ROW, [(i, 31 - i) for i in range(32)])
    mirror_after = lax.ppermute(own, ROW, [(i, (32 - i) % 32) for i in range(32)])
    pieces = sent_to_all(piece, ROW)
    cov, cov_near, mapped = covariance_block(
        own, after, mirror, mirror_after, tail, pieces, start_basis
    )
    mapped = total_over(mapped, ROW)
    (terms,) = local_call(image_kernel, [(3 * K // 2, BLOCK)], mapped, cov_near)
    both = lax.all_gather(terms.reshape(2, 3 * K // 4, BLOCK), "core")
    mine = lax.dynamic_index_in_dim(both, core, 1, keepdims=False).sum(axis=0)
    mine = sent_to_all(mine, "z").sum(axis=0)
    total = lax.all_gather(mine, "core", tiled=True)
    mapped, grams = local_call(first_factor_kernel, [(K, BLOCK), (4, K // 2, 2 * K)], total)
    grams = sent_to_all(exchanged(grams, "row_0").sum(axis=0), "row_1")
    (basis,) = local_call(last_factor_kernel, [(K, BLOCK)], grams, mapped, result=jax.ShapeDtypeStruct)
    return (cov, basis)


def solution(mesh):
    split = Mesh(mesh.devices.reshape(4, 8, 8, 2), EVERY)
    in_specs = (P(ROW, None, None), P(), P(SHIFT), P(None, ROW))
    out_specs = (P(ROW, SHIFT), P(None, ROW))
    return jax.shard_map(
        per_device, mesh=split, in_specs=in_specs, out_specs=out_specs, check_vma=False
    )
```

```python
import jax
import jax.numpy as jnp
from jax import lax
from jax.experimental import pallas as pl
from jax.experimental.pallas import tpu as pltpu
from jax.sharding import Mesh
from jax.sharding import PartitionSpec as P


K = 64
SNAPS = 128
SHIFTS = 48
BLOCK = 128
GROUP = 16
ROW = ("row_0", "row_1")
SHIFT = ("z", "core")
EVERY = (*ROW, *SHIFT)
HALF_ROOT = 0.7071067811865476
HIGH = lax.Precision.HIGHEST


def dot_nt(a, b, precision=None):
    return lax.dot_general(
        a, b, (((1,), (1,)), ((), ())), precision=precision, preferred_element_type=jnp.float32
    )


def dot_nn(a, b, precision=None):
    return lax.dot_general(
        a, b, (((1,), (0,)), ((), ())), precision=precision, preferred_element_type=jnp.float32
    )


def near(x):
    return pltpu.with_memory_space_constraint(x, pltpu.VMEM)


def sent_to_all(x, axis):
    copies = jnp.broadcast_to(x, (lax.axis_size(axis), *x.shape))
    return lax.all_to_all(copies, axis, split_axis=0, concat_axis=0, tiled=True)


def copies_kernel(piece, copies):
    for i in range(copies.shape[0]):
        copies[i] = piece[...]


def copies_of(piece, count):
    return pl.pallas_call(
        copies_kernel, name="copies", out_shape=pltpu.VMEM((count, *piece.shape), piece.dtype)
    )(near(piece))


def covariance_kernel(
    own, after, mirror, mirror_after, tail, pieces, basis,
    cov, cov_near, mapped, row_w, row_z, col_w, col_z, acc,
):
    r = lax.axis_index(ROW)
    c = lax.axis_index(SHIFT)
    offsets = []
    for q in range(16):
        held = pieces[q, 16:, :SNAPS].astype(jnp.float32).astype(jnp.int32)
        offsets += [held[i, 0] for i in range(3)]
    flip = (
        lax.broadcasted_iota(jnp.int32, (BLOCK, BLOCK), 0)
        + lax.broadcasted_iota(jnp.int32, (BLOCK, BLOCK), 1)
        == BLOCK - 1
    ).astype(jnp.bfloat16)

    def put_window(ref, at, block, upper):
        re = block[:, :SNAPS].astype(jnp.float32) * HALF_ROOT
        im = block[:, SNAPS:].astype(jnp.float32) * HALF_ROOT
        ref[0, pl.ds(at, BLOCK), :] = jnp.where(upper, re, im)
        ref[1, pl.ds(at, BLOCK), :] = jnp.where(upper, im, -re)

    def put_mirror(ref, at, block, upper):
        turned = dot_nn(flip, block) * HALF_ROOT
        re = turned[:, :SNAPS]
        im = turned[:, SNAPS:]
        ref[0, pl.ds(at, BLOCK), :] = jnp.where(upper, re, -im)
        ref[1, pl.ds(at, BLOCK), :] = jnp.where(upper, im, re)

    row_upper = r < 16
    put_window(row_w, 0, own[...], row_upper)
    put_window(row_w, BLOCK, jnp.where(r == 31, tail[...], after[...]), row_upper)
    put_mirror(row_z, 0, jnp.where(r == 0, tail[...], mirror_after[...]), row_upper)
    put_mirror(row_z, BLOCK, mirror[...], row_upper)

    odd = [jnp.concatenate([pieces[2 * i + j, :16, :] for i in range(8)], axis=0) for j in range(2)]
    even = [jnp.concatenate([pieces[16 + 4 * i + j] for i in range(4)], axis=0) for j in range(4)]
    col_upper = c < 8
    put_window(col_w, 0, even[0], col_upper)
    put_window(col_w, BLOCK, odd[0], col_upper)
    put_window(col_w, 2 * BLOCK, jnp.where(c == 15, tail[...], even[2]), col_upper)
    put_mirror(col_z, 0, jnp.where(c == 0, tail[...], even[3]), col_upper)
    put_mirror(col_z, BLOCK, odd[1], col_upper)
    put_mirror(col_z, 2 * BLOCK, even[1], col_upper)

    acc[...] = jnp.zeros(acc.shape, jnp.float32)

    def step(carry):
        left, right = [], []
        for u in range(3 * GROUP):
            o = offsets[u]
            for plane in range(2):
                left.append(
                    (row_w[plane, pl.ds(o, BLOCK), :] + row_z[plane, pl.ds(BLOCK - o, BLOCK), :])
                    .astype(jnp.bfloat16)
                )
                right.append(
                    (col_w[plane, pl.ds(o, 2 * BLOCK), :] + col_z[plane, pl.ds(BLOCK - o, 2 * BLOCK), :])
                    .astype(jnp.bfloat16)
                )
        acc[...] += dot_nt(jnp.concatenate(left, axis=1), jnp.concatenate(right, axis=1))
        return carry

    step(0)
    block = acc[...] * (1.0 / (SNAPS * SHIFTS))
    cov[...] = block
    cov_near[...] = block
    image = dot_nn(basis[...], block, HIGH)
    for p in range(32):
        mapped[p] = image[4 * (p // 2) : 4 * (p // 2) + 4, SNAPS * (p % 2) : SNAPS * (p % 2) + SNAPS]


def covariance_block(own, after, mirror, mirror_after, tail, pieces, basis):
    vmem = pl.BlockSpec(memory_space=pltpu.VMEM)
    return pl.pallas_call(
        covariance_kernel,
        name="covariance_block",
        in_specs=[vmem] * 7,
        out_specs=[vmem] * 3,
        out_shape=[
            jax.ShapeDtypeStruct((BLOCK, 2 * BLOCK), jnp.float32),
            pltpu.VMEM((BLOCK, 2 * BLOCK), jnp.float32),
            pltpu.VMEM((32, 4, SNAPS), jnp.float32),
        ],
        scratch_shapes=[
            pltpu.VMEM((2, 2 * BLOCK, SNAPS), jnp.float32),
            pltpu.VMEM((2, 2 * BLOCK, SNAPS), jnp.float32),
            pltpu.VMEM((2, 3 * BLOCK, SNAPS), jnp.float32),
            pltpu.VMEM((2, 3 * BLOCK, SNAPS), jnp.float32),
            pltpu.VMEM((BLOCK, 2 * BLOCK), jnp.float32),
        ],
    )(*[near(x) for x in (own, after, mirror, mirror_after, tail, pieces, basis)])


def inverse_factor(gram):
    row_at = lax.broadcasted_iota(jnp.int32, (8, 2 * K), 0)
    lane_at = lax.broadcasted_iota(jnp.int32, (8, 2 * K), 1)
    tiles, done = [], []
    for t in range(K // 8):
        part = gram[8 * t : 8 * t + 8]
        eye = (lane_at == row_at + (K + 8 * t)).astype(jnp.float32)
        tiles.append(jnp.where(lane_at < K, jnp.concatenate([part, part], axis=1), eye))
        done.append(jnp.zeros((8, 2 * K), jnp.float32))
    for at in range(K // 8):
        own, rest = at, range(at + 1, K // 8)
        cols = [
            [jnp.broadcast_to(tiles[t][:, j : j + 1], (8, 2 * K)) for t in range(at, K // 8)]
            for j in range(8 * at, 8 * at + 8)
        ]
        for s in range(8):
            col = cols[s]
            below = row_at > s
            pivot = col[0][s : s + 1, :]
            inverse = 1.0 / pivot
            row = tiles[own][s : s + 1, :]
            scaled = row * inverse
            done[own] = jnp.where(row_at == s, row / jnp.sqrt(pivot), done[own])
            for k in range(s + 1, 8):
                share = cols[k][0][s : s + 1, :] * inverse
                left = [c - f * share for c, f in zip(cols[k], col)]
                left[0] = jnp.where(below, left[0], cols[k][0])
                cols[k] = left
            tiles[own] = jnp.where(below, tiles[own] - col[0] * scaled, tiles[own])
            for t in rest:
                tiles[t] = tiles[t] - col[t - at] * scaled
    return jnp.concatenate(done, axis=0)[:, K:]


def image_kernel(mapped, cov, terms):
    image = jnp.concatenate(
        [jnp.concatenate([mapped[2 * i], mapped[2 * i + 1]], axis=1) for i in range(16)], axis=0
    )
    terms[:K] = dot_nt(image, cov[...], HIGH)
    terms[K:] = halves_side_by_side(dot_nt(image, image, HIGH))


def halves_side_by_side(gram):
    return jnp.concatenate([gram[: K // 2], gram[K // 2 :]], axis=1)


def halves_stacked(packed):
    return jnp.concatenate([packed[:, :K], packed[:, K:]], axis=0)


def first_factor_kernel(total, mapped, grams):
    image = dot_nn(inverse_factor(halves_stacked(total[K:])), total[:K], HIGH)
    mapped[...] = image
    part = halves_side_by_side(dot_nt(image, image, HIGH))
    for i in range(grams.shape[0]):
        grams[i] = part


def last_factor_kernel(grams, mapped, basis):
    total = jnp.sum(grams[...], axis=0)
    basis[...] = dot_nn(inverse_factor(halves_stacked(total)), mapped[...], HIGH)


def local_call(kernel, shapes, *operands, result=pltpu.VMEM):
    spaces = [pltpu.SMEM if x.dtype == jnp.int32 else pltpu.VMEM for x in operands]
    return pl.pallas_call(
        kernel,
        in_specs=[pl.BlockSpec(memory_space=space) for space in spaces],
        out_shape=[result(s, jnp.float32) for s in shapes],
    )(*[x if x.dtype == jnp.int32 else near(x) for x in operands])


def exchanged(tiles, axis):
    return lax.all_to_all(tiles, axis, split_axis=0, concat_axis=0, tiled=True)


def total_over(tiles, axis):
    return sent_to_all(exchanged(tiles, axis).sum(axis=0), axis)


def piece_routes():
    routes = []
    for b in range(32):
        for q in range(16):
            if b % 2:
                c = (b - 1) // 2 if q % 2 == 0 else (31 - b) // 2
                to = q
            else:
                c = (b // 2, (30 - b) // 2, (b // 2 - 1) % 16, (16 - b // 2) % 16)[q % 4]
                to = q + 16
            routes.append((b * 16 + q, to * 16 + c))
    return routes


def per_device(snapshots, tail_sensors, shift_offsets, start_basis):
    r = lax.axis_index(ROW)
    c = lax.axis_index(SHIFT)
    tail = tail_sensors.reshape(BLOCK, 2 * SNAPS)
    offsets = jnp.zeros((16, 2 * SNAPS), jnp.bfloat16)
    offsets = lax.dynamic_update_slice(offsets, shift_offsets.astype(jnp.bfloat16)[:, None], (0, 0))
    core = lax.axis_index("core").astype(jnp.uint32)
    own, core, offsets = lax.optimization_barrier((snapshots, core, offsets))
    own = own.reshape(BLOCK, 2 * SNAPS)
    odd_piece = jnp.concatenate([lax.dynamic_slice_in_dim(own, 16 * (c // 2), 16, 0), offsets], 0)
    even_piece = lax.dynamic_slice_in_dim(own, 32 * (c // 4), 32, 0)
    piece = jnp.where(r % 2 == 1, odd_piece, even_piece)
    piece = lax.ppermute(piece, EVERY, piece_routes())
    after = lax.ppermute(own, ROW, [(i, (i - 1) % 32) for i in range(32)])
    mirror = lax.ppermute(own, ROW, [(i, 31 - i) for i in range(32)])
    mirror_after = lax.ppermute(own, ROW, [(i, (32 - i) % 32) for i in range(32)])
    pieces = exchanged(copies_of(piece, lax.axis_size(ROW)), ROW)
    cov, cov_near, mapped = covariance_block(
        own, after, mirror, mirror_after, tail, pieces, start_basis
    )
    mapped = total_over(mapped, ROW)
    (terms,) = local_call(image_kernel, [(3 * K // 2, BLOCK)], mapped, cov_near)
    both = lax.all_gather(terms.reshape(2, 3 * K // 4, BLOCK), "core")
    mine = lax.dynamic_index_in_dim(both, core, 1, keepdims=False).sum(axis=0)
    mine = sent_to_all(mine, "z").sum(axis=0)
    total = lax.all_gather(mine, "core", tiled=True)
    mapped, grams = local_call(first_factor_kernel, [(K, BLOCK), (8, K // 2, 2 * K)], total)
    grams = sent_to_all(exchanged(grams, "row_1").sum(axis=0), "row_0")
    (basis,) = local_call(last_factor_kernel, [(K, BLOCK)], grams, mapped, result=jax.ShapeDtypeStruct)
    return (cov, basis)


def solution(mesh):
    split = Mesh(mesh.devices.reshape(4, 8, 8, 2), EVERY)
    in_specs = (P(ROW, None, None), P(), P(SHIFT), P(None, ROW))
    out_specs = (P(ROW, SHIFT), P(None, ROW))
    return jax.shard_map(
        per_device, mesh=split, in_specs=in_specs, out_specs=out_specs, check_vma=False
    )
```
